32 devices in a mesh: col: 8 (over y, x, core), row: 4 (over z).
Axes of the slice: x: 2, y: 2, z: 4, core: 2. Of those that a mesh axis runs over, the one named last changes fastest.
Arguments:
- visibilities: bfloat16 [2, 8192, 4096], P(None, 'col', 'row'), may hold values from -6 to 6
- col_offsets: int32 [8], P('col'), may hold values from 0 to 15360
- row_offsets: int32 [4], replicated, may hold values from 0 to 15360
- facet_offsets: int32 [8, 2], replicated, may hold values from 0 to 16383
- facet_order: int32 [8], replicated, may hold values from 0 to 7, each once
- vis_counts: int32 [8, 4], P('col', 'row'), may hold values from 512 to 1024
Outputs:
- facet_images: float32 [8, 2, 64, 4096], P('col', None, None, 'row')
- peak: float32 [8], P('col')
The draws below stay inside these ranges and needn't reach their ends.
Inputs may be any that keep to these rules, and one draw needn't show every extreme that they name: `facet_order`: each slot names a different facet.
All inputs are finite; a program needn't handle non-finite values.
Results may differ from the reference program's by a relative error of at most 0.0078.
Values may be sent and summed in bfloat16 or wider, within the bound.
No kernel may reach another device: no remote copies, remote signals or barrier semaphores. Data moves between devices by JAX's collectives and lax.ppermute only.
A program may use at most 128 MiB of HBM per device.

```python
import math
import jax
import jax.numpy as jnp
from jax import lax

M = 1024
FS = 4096
NG = 16384
FR = 64
NFACET = 8
N_COL = 8
N_ROW = 4


def with_ends(entries, rng, least, largest):
    extent = entries.shape
    place = [jax.random.randint(jax.random.fold_in(rng, axis), (), 0, extent[axis]) for axis in range(len(extent))]
    entries = entries.at[tuple(place)].set(least)
    longest = extent.index(max(extent))
    place[longest] = (place[longest] + 1) % extent[longest]
    return entries.at[tuple(place)].set(largest)


def steps_of(key, dims, pieces, low, high):
    gain = 1.0
    for dim, blocks in pieces:
        steps = jax.random.uniform(jax.random.fold_in(jax.random.fold_in(key, 6), dim), (blocks,), jnp.float32, low / len(pieces), high / len(pieces))
        gain = gain * jnp.repeat(jnp.exp(steps), dims[dim] // blocks).reshape((-1,) + (1,) * (len(dims) - 1 - dim))
    return gain


def noise(own_key, shape, width, reach, cuts=(), kind=jnp.bfloat16):
    result = jax.random.normal(own_key, shape, jnp.float32) * width
    if len(cuts) > 0:
        result = steps_of(own_key, shape, cuts, -0.22, 0.18) * result
    return jnp.clip(result, min=-reach, max=reach).astype(kind)


def setup_inputs(seed: int = 0) -> dict:
    arg_keys = jax.random.split(jax.random.key(seed), 7)
    return {
        "visibilities": noise(arg_keys[0], (2, N_COL * M, N_ROW * M), 1.0, 6.0, ((1, 8), (2, 4))),
        "col_offsets": with_ends(jax.random.randint(arg_keys[1], (N_COL,), 0, NG - M + 1), jax.random.fold_in(arg_keys[1], 1), 0, NG - M).astype(jnp.int32),
        "row_offsets": with_ends(jax.random.randint(arg_keys[2], (N_ROW,), 0, NG - M + 1), jax.random.fold_in(arg_keys[2], 1), 0, NG - M).astype(jnp.int32),
        "facet_offsets": with_ends(jax.random.randint(arg_keys[3], (NFACET, 2), 0, NG), jax.random.fold_in(arg_keys[3], 1), 0, NG - 1).astype(jnp.int32),
        "facet_order": jax.random.permutation(arg_keys[4], NFACET).astype(jnp.int32),
        "vis_counts": with_ends(jax.random.randint(arg_keys[5], (N_COL, N_ROW), M // 2, M + 1), jax.random.fold_in(arg_keys[5], 1), M // 2, M).astype(jnp.int32),
    }


TWO_PI = 2.0 * math.pi
BEAM_SLOPE = 0.66

def phase_table(first_ids, second_ids, factor):
    product = first_ids[:, None] * second_ids[None, :] % NG
    angles = product.astype(jnp.float32) * (TWO_PI / NG)
    return ((jnp.cos(angles) * factor).astype(jnp.bfloat16), (jnp.sin(angles) * factor).astype(jnp.bfloat16))

def complex_product(left_real, left_imag, right_real, right_imag):
    left_rows = jnp.concatenate([left_real, left_imag], axis=0)
    right_cols = jnp.concatenate([right_real, right_imag], axis=1)
    product = jnp.dot(left_rows, right_cols, preferred_element_type=jnp.float32)
    product = product.reshape(2, left_real.shape[0], 2, right_real.shape[1])
    real_part = product[0, :, 0] - product[1, :, 1]
    imag_part = product[0, :, 1] + product[1, :, 0]
    return (real_part, imag_part)

def reference(visibilities, col_offsets, row_offsets, facet_offsets, facet_order, vis_counts):
    slot_pick = (facet_order[:, None] == jnp.arange(NFACET, dtype=jnp.int32)[None, :]).astype(jnp.int32)
    slot_offsets = lax.optimization_barrier(jnp.sum(slot_pick[:, :, None] * facet_offsets[None, :, :], axis=1))
    row_ids = jnp.arange(M, dtype=jnp.int32)
    pixel_rows = jnp.arange(FR, dtype=jnp.int32) + (FS // 2 - FR // 2)
    pixel_cols = jnp.arange(FS, dtype=jnp.int32)
    grid_u = (col_offsets[:, None] + row_ids[None, :]).reshape(N_COL * M)
    first_scale = 1.0 / math.sqrt(M * N_COL)
    second_scale = 0.5 / math.sqrt(M * N_ROW)

    def add_row(running, row_index):
        column_strip = lax.dynamic_slice_in_dim(visibilities, (row_index * M).astype(jnp.int32), M, 2)
        counts_here = lax.dynamic_index_in_dim(vis_counts, row_index, 1, keepdims=False)
        live_rows = (row_ids[None, :] < counts_here[:, None]).reshape(N_COL * M)
        column_strip = jnp.where(live_rows[None, :, None], column_strip, jnp.zeros_like(column_strip))
        grid_v = lax.dynamic_index_in_dim(row_offsets, row_index, 0, keepdims=False) + row_ids

        def one_slot(slot_index):
            offsets = lax.dynamic_index_in_dim(slot_offsets, slot_index, 0, keepdims=False)
            image_rows = (offsets[0] + pixel_rows) % NG
            table_real, table_imag = phase_table(image_rows, grid_u, first_scale)
            part_real, part_imag = complex_product(table_real, table_imag, column_strip[0], column_strip[1])
            columns = jnp.stack([part_real, part_imag], axis=0).astype(jnp.bfloat16)
            image_cols = (offsets[1] + pixel_cols) % NG
            second_real, second_imag = phase_table(grid_v, image_cols, second_scale)
            out_real, out_imag = complex_product(columns[0], columns[1], second_real, second_imag)
            return jnp.stack([out_real, out_imag], axis=0)
        return (running + lax.map(one_slot, jnp.arange(NFACET, dtype=jnp.int32)), None)
    initial = jnp.zeros((NFACET, 2, FR, FS), jnp.float32)
    facet_sum, ignored = lax.scan(add_row, initial, jnp.arange(N_ROW, dtype=jnp.int32))
    beam = 1.0 - BEAM_SLOPE * (pixel_cols.astype(jnp.float32) + 0.5) / FS
    facet_images = facet_sum / beam[None, None, None, :]
    magnitude = jnp.sqrt(facet_images[:, 0] * facet_images[:, 0] + facet_images[:, 1] * facet_images[:, 1])
    peak = lax.optimization_barrier(jnp.max(magnitude, axis=(1, 2)))
    return (facet_images, peak)
```

```python
import functools
import math

import jax
import jax.numpy as jnp
from jax import lax
from jax.experimental import pallas as pl
from jax.experimental.pallas import tpu as pltpu
from jax.sharding import PartitionSpec as P

FS = 4096
NG = 16384
FR = 64
BEAM_SLOPE = 0.66
LANES = 128
TILE = 8
MIB = 1 << 20
VMEM = pl.BlockSpec(memory_space=pltpu.VMEM)
SMEM = pl.BlockSpec(memory_space=pltpu.SMEM)
HBM = pl.BlockSpec(memory_space=pl.ANY)


def cis(phase):
    quarter = NG // 4
    turned = phase + quarter // 2
    quadrant = (turned & (NG - 1)) // quarter
    rest = (turned & (quarter - 1)) - quarter // 2
    t = rest.astype(jnp.float32) * (2.0 * math.pi / NG)
    t2 = t * t
    s = t * (1 + t2 * (-1 / 6 + t2 * (1 / 120 + t2 * (-1 / 5040 + t2 * (1 / 362880)))))
    c = 1 + t2 * (-1 / 2 + t2 * (1 / 24 + t2 * (-1 / 720 + t2 * (1 / 40320))))
    odd = (quadrant & 1) == 1
    real = jnp.where(odd, s, c)
    imag = jnp.where(odd, c, s)
    real = jnp.where((quadrant == 1) | (quadrant == 2), -real, real)
    imag = jnp.where(quadrant >= 2, -imag, imag)
    return real, imag


def times(a, b):
    return a[0] * b[0] - a[1] * b[1], a[0] * b[1] + a[1] * b[0]


def iota(shape, dim):
    return lax.broadcasted_iota(jnp.int32, shape, dim)


def stacked_rows(values, height):
    row = iota((height, 1), 0)
    result = jnp.zeros((height, 1), jnp.int32)
    for k, value in enumerate(values):
        result = jnp.where(row == k, value, result)
    return result


def store_stacked(ref, row, high, depth, real, imag):
    h = real.shape[0]
    real, imag, minus = (x.astype(jnp.bfloat16) for x in (real, imag, -imag))
    ref[row : row + h, :depth] = real
    ref[row : row + h, depth:] = minus
    ref[row + high : row + high + h, :depth] = imag
    ref[row + high : row + high + h, depth:] = real


def column_kernel(flip, slots, scale, offs, order, col, count, vis, out, table, fine):
    depth = vis.shape[1]

    @pl.when(pl.program_id(0) == 0)
    def build():
        c = lax.axis_index("col")
        lane = iota((TILE, depth), 1)
        sub = iota((TILE, depth), 0)
        u = col[0] + lane
        few = cis(u * sub)
        many = cis(u * (sub * TILE))
        starts = []
        for k in range(slots):
            slot = (((c // 2) ^ k) * 2) + ((c % 2) ^ flip)
            starts.append((offs[order[slot], 0] + (FS // 2 - FR // 2)) % NG)
        height = -(-slots // TILE) * TILE
        xs = cis((col[0] + iota((height, depth), 1)) * stacked_rows(starts, height))
        live = jnp.where(iota((height, depth), 1) < count[0, 0], scale, 0.0)
        xs = (xs[0] * live, xs[1] * live)
        for k in range(slots):
            x = tuple(jnp.broadcast_to(v[k : k + 1], (TILE, depth)) for v in xs)
            xa = times(x, many)
            fine[0], fine[1] = xa
            for a in range(0, FR // TILE, 2):
                parts = []
                for step in range(2):
                    row = tuple(
                        jnp.broadcast_to(fine[z, a + step : a + step + 1, :], (TILE, depth)) for z in range(2)
                    )
                    parts.append(times(row, few))
                real = jnp.concatenate([parts[0][0], parts[1][0]], axis=0)
                imag = jnp.concatenate([parts[0][1], parts[1][1]], axis=0)
                store_stacked(table, k * 2 * FR + a * TILE, FR, depth, real, imag)

    right = vis[...].reshape(2 * depth, vis.shape[2])
    out[...] = jnp.dot(table[...], right, preferred_element_type=jnp.float32).astype(out.dtype)


def columns_of(flip, slots, scale, offs, order, col, count, vis):
    _, depth, width = vis.shape
    block = 256
    rows = slots * 2 * FR
    return pl.pallas_call(
        functools.partial(column_kernel, flip, slots, scale),
        grid=(width // block,),
        in_specs=[SMEM, SMEM, SMEM, SMEM, pl.BlockSpec((2, depth, block), lambda n: (0, 0, n))],
        out_specs=pl.BlockSpec((rows, block), lambda n: (0, n)),
        out_shape=jax.ShapeDtypeStruct((rows, width), jnp.bfloat16),
        scratch_shapes=[
            pltpu.VMEM((rows, 2 * depth), jnp.bfloat16),
            pltpu.VMEM((2, TILE, depth), jnp.float32),
        ],
        compiler_params=pltpu.CompilerParams(vmem_limit_bytes=20 * MIB),
        cost_estimate=pl.CostEstimate(
            flops=rows * 4 * depth * width, bytes_accessed=4 * depth * width, transcendentals=0
        ),
        name=f"columns_{flip}",
    )(offs, order, col, count, vis)


def wave_kernel(after, out):
    del after
    depth, width = out.shape[0] // 2, out.shape[1]
    lane = iota((TILE, width), 1)
    sub = iota((TILE, width), 0)
    few = cis(lane * sub)

    def body(block, carry):
        coarse = cis(lane * ((block * TILE + sub) * TILE))
        base = block * (TILE * TILE)
        for a in range(0, TILE, 2):
            parts = [
                times(tuple(jnp.broadcast_to(v[a + s : a + s + 1], (TILE, width)) for v in coarse), few)
                for s in range(2)
            ]
            row = pl.multiple_of(base + a * TILE, 2 * TILE)
            for z in range(2):
                value = jnp.concatenate([parts[0][z], parts[1][z]], axis=0)
                out[pl.ds(row + z * depth, 2 * TILE), :] = value.astype(out.dtype)
        return carry

    lax.fori_loop(0, depth // (TILE * TILE), body, 0)


def waves(after, depth, width):
    return pl.pallas_call(
        wave_kernel,
        in_specs=[HBM],
        out_specs=VMEM,
        out_shape=jax.ShapeDtypeStruct((2 * depth, width), jnp.bfloat16),
        compiler_params=pltpu.CompilerParams(vmem_limit_bytes=20 * MIB),
        cost_estimate=pl.CostEstimate(flops=4 * 10**9, bytes_accessed=4 * depth * width, transcendentals=0),
        name="waves",
    )(after)


def row_kernel(scale, rows, offs, order, roff, *refs):
    pieces, wave, outs = refs[:rows], refs[rows], refs[rows + 1 : 2 * rows + 1]
    left, turned = refs[2 * rows + 1 :]
    depth = pieces[0].shape[1]
    high = pieces[0].shape[0] // 2
    width = wave.shape[1]
    r = lax.axis_index("row")
    start = offs[order[lax.axis_index("col")], 1]
    height = -(-rows // TILE) * TILE
    sources = [roff[r ^ p] for p in range(rows)]
    blocks = stacked_rows([(start + (r ^ b) * width) % NG for b in range(rows)], height)
    for p in range(rows):
        phase = cis((sources[p] + iota((height, depth), 1)) * blocks)
        turned[0], turned[1] = phase[0] * scale, phase[1] * scale
        value = pieces[p][...].astype(jnp.float32)
        value = (value[:high], value[high:])
        for b in range(rows):
            turn = tuple(jnp.broadcast_to(turned[z, b : b + 1, :], (high, depth)) for z in range(2))
            real, imag = times(value, turn)
            store_stacked(left, (p * rows + b) * 2 * high, high, depth, real, imag)
    lane = iota((height, width), 1)
    after = cis(lane * stacked_rows(sources, height))
    piece = min(2 * LANES, width)
    largest = jnp.zeros((high, LANES), jnp.float32)
    for n in range(0, width, piece):
        product = jnp.dot(left[...], wave[:, n : n + piece], preferred_element_type=jnp.float32)
        for b in range(rows):
            real = imag = None
            for p in range(rows):
                at = (p * rows + b) * 2 * high
                value = (product[at : at + high], product[at + high : at + 2 * high])
                turn = tuple(v[p : p + 1, n : n + piece] for v in after)
                x, y = times(value, turn)
                real = x if real is None else real + x
                imag = y if imag is None else imag + y
            j = ((r ^ b) * width + n + iota((1, piece), 1)).astype(jnp.float32)
            beam = 1.0 / (1.0 - BEAM_SLOPE * (j + 0.5) / FS)
            real = real * beam
            imag = imag * beam
            power = real * real + imag * imag
            for m in range(0, piece, LANES):
                at = (n + m) // LANES * 2 * high
                outs[b][at : at + high] = real[:, m : m + LANES].astype(jnp.bfloat16)
                outs[b][at + high : at + 2 * high] = imag[:, m : m + LANES].astype(jnp.bfloat16)
                largest = jnp.maximum(largest, power[:, m : m + LANES])
    peak = jnp.broadcast_to(jnp.sqrt(jnp.max(largest, keepdims=True)), (2 * TILE, LANES))
    first = peak.astype(jnp.bfloat16).astype(jnp.float32)
    second = (peak - first).astype(jnp.bfloat16).astype(jnp.float32)
    third = peak - first - second
    sub = iota((2 * TILE, LANES), 0)
    peak = jnp.where(sub == 0, first, jnp.where(sub == 1, second, jnp.where(sub == 2, third, 0.0)))
    for b in range(rows):
        outs[b][width // LANES * 2 * high :] = peak.astype(jnp.bfloat16)


def rows_of(scale, offs, order, roff, pieces, wave):
    rows = len(pieces)
    double, depth = pieces[0].shape
    width = wave.shape[1]
    shape = jax.ShapeDtypeStruct((width // LANES * double + 2 * TILE, LANES), jnp.bfloat16)
    return pl.pallas_call(
        functools.partial(row_kernel, scale, rows),
        in_specs=[SMEM] * 3 + [VMEM] * (rows + 1),
        out_specs=[VMEM] * rows,
        out_shape=[shape] * rows,
        scratch_shapes=[
            pltpu.VMEM((rows * rows * double, 2 * depth), jnp.bfloat16),
            pltpu.VMEM((2, -(-rows // TILE) * TILE, depth), jnp.float32),
        ],
        compiler_params=pltpu.CompilerParams(vmem_limit_bytes=32 * MIB),
        cost_estimate=pl.CostEstimate(
            flops=rows * rows * double * 4 * depth * width, bytes_accessed=4 * depth * width, transcendentals=0
        ),
        name="rows",
    )(offs, order, roff, *pieces, wave)


def finish_kernel(rows, *refs):
    pieces, (image, peak) = refs[:rows], refs[rows:]
    width = image.shape[3]
    high = image.shape[2] // rows
    r = lax.axis_index("row")
    largest = None
    for p in range(rows):
        for n in range(0, width, LANES):
            row = n // LANES * 2 * high
            if high % TILE == 0:
                at = pl.ds(pl.multiple_of((r ^ p) * high, high), high)
                value = pieces[p][row : row + 2 * high, :].astype(jnp.float32)
            else:
                at = pl.ds(p * high, high)
                value = pieces[0][row : row + 2 * high, :].astype(jnp.float32)
                for q in range(1, rows):
                    other = pieces[q][row : row + 2 * high, :].astype(jnp.float32)
                    value = jnp.where((r ^ p) == q, other, value)
            image[0, 0, at, n : n + LANES] = value[:high]
            image[0, 1, at, n : n + LANES] = value[high:]
        parts = pieces[p][width // LANES * 2 * high :, :].astype(jnp.float32)
        value = (parts[0:1] + parts[1:2]) + parts[2:3]
        largest = value if largest is None else jnp.maximum(largest, value)
    peak[0] = jnp.max(largest)


def finish(pieces, width):
    rows = len(pieces)
    return pl.pallas_call(
        functools.partial(finish_kernel, rows),
        in_specs=[VMEM] * rows,
        out_specs=[VMEM, SMEM],
        out_shape=[
            jax.ShapeDtypeStruct((1, 2, FR, width), jnp.float32),
            jax.ShapeDtypeStruct((1,), jnp.float32),
        ],
        compiler_params=pltpu.CompilerParams(vmem_limit_bytes=16 * MIB),
        name="finish",
    )(*pieces)


def local(visibilities, col_offsets, row_offsets, facet_offsets, facet_order, vis_counts):
    cols = lax.axis_size("col")
    rows = lax.axis_size("row")
    _, depth, width = visibilities.shape
    slots = cols // 2
    high = FR // rows
    scalars = (facet_offsets, facet_order, col_offsets, vis_counts)
    first_scale = 1.0 / math.sqrt(depth * cols)
    second_scale = 0.5 / math.sqrt(width * rows)

    def swap(value, axis, count, bit):
        return lax.ppermute(value, axis, [(i, i ^ bit) for i in range(count)])

    given = columns_of(1, slots, first_scale, *scalars, visibilities)
    taken = swap(given, "col", cols, 1)
    mine = columns_of(0, slots, first_scale, *scalars, visibilities)
    pair = (mine.astype(jnp.float32) + taken.astype(jnp.float32)).reshape(slots, 2 * FR, width)
    total = pair[0]
    sent = [swap(pair[k].astype(jnp.bfloat16), "col", cols, 2 * k) for k in range(1, slots)]
    wave = waves(mine, width, FS // rows)
    for value in sent:
        total = total + value.astype(jnp.float32)
    total = total.astype(jnp.bfloat16).reshape(2, FR, width)
    r = lax.axis_index("row")
    pieces = []
    for p in range(rows):
        part = lax.dynamic_slice_in_dim(total, (r ^ p) * high, high, 1).reshape(2 * high, width)
        pieces.append(part if p == 0 else swap(part, "row", rows, p))
    parts = rows_of(second_scale, facet_offsets, facet_order, row_offsets, pieces, wave)
    parts = [part if p == 0 else swap(part, "row", rows, p) for p, part in enumerate(parts)]
    image, peak = finish(parts, FS // rows)
    return image, peak


def solution(mesh):
    in_specs = (P(None, "col", "row"), P("col"), P(), P(), P(), P("col", "row"))
    out_specs = (P("col", None, None, "row"), P("col"))
    return jax.shard_map(local, mesh=mesh, in_specs=in_specs, out_specs=out_specs, check_vma=False)
```

```python
import functools
import math

import jax
import jax.numpy as jnp
from jax import lax
from jax.experimental import pallas as pl
from jax.experimental.pallas import tpu as pltpu
from jax.sharding import PartitionSpec as P

FS = 4096
NG = 16384
FR = 64
BEAM_SLOPE = 0.66
LANES = 128
TILE = 8
MIB = 1 << 20
VMEM = pl.BlockSpec(memory_space=pltpu.VMEM)
SMEM = pl.BlockSpec(memory_space=pltpu.SMEM)
HBM = pl.BlockSpec(memory_space=pl.ANY)


def cis(phase):
    quarter = NG // 4
    turned = phase + quarter // 2
    quadrant = (turned & (NG - 1)) // quarter
    rest = (turned & (quarter - 1)) - quarter // 2
    t = rest.astype(jnp.float32) * (2.0 * math.pi / NG)
    t2 = t * t
    s = t * (1 + t2 * (-1 / 6 + t2 * (1 / 120 + t2 * (-1 / 5040 + t2 * (1 / 362880)))))
    c = 1 + t2 * (-1 / 2 + t2 * (1 / 24 + t2 * (-1 / 720 + t2 * (1 / 40320))))
    odd = (quadrant & 1) == 1
    real = jnp.where(odd, s, c)
    imag = jnp.where(odd, c, s)
    real = jnp.where((quadrant == 1) | (quadrant == 2), -real, real)
    imag = jnp.where(quadrant >= 2, -imag, imag)
    return real, imag


def times(a, b):
    return a[0] * b[0] - a[1] * b[1], a[0] * b[1] + a[1] * b[0]


def iota(shape, dim):
    return lax.broadcasted_iota(jnp.int32, shape, dim)


def stacked_rows(values, height):
    row = iota((height, 1), 0)
    result = jnp.zeros((height, 1), jnp.int32)
    for k, value in enumerate(values):
        result = jnp.where(row == k, value, result)
    return result


def store_stacked(ref, row, high, depth, real, imag):
    h = real.shape[0]
    real, imag, minus = (x.astype(jnp.bfloat16) for x in (real, imag, -imag))
    ref[row : row + h, :depth] = real
    ref[row : row + h, depth:] = minus
    ref[row + high : row + high + h, :depth] = imag
    ref[row + high : row + high + h, depth:] = real


def in_hbm(*arrays):
    return [pltpu.with_memory_space_constraint(x, pltpu.HBM) for x in arrays]


def small_copies(sources, targets, sems):
    return [pltpu.make_async_copy(s, t, sems.at[k]) for k, (s, t) in enumerate(zip(sources, targets))]


def build_table(table, small, first, slots, depth):
    few = (small[0], small[1])
    many = (small[2], small[3])
    for k in range(slots):
        k0, k1 = divmod(first + k, TILE)
        x = tuple(jnp.broadcast_to(small[4 + 2 * k0 + z, k1 : k1 + 1, :], (TILE, depth)) for z in range(2))
        xa = times(x, many)
        for a in range(0, FR // TILE, 2):
            parts = [
                times(tuple(jnp.broadcast_to(v[a + t : a + t + 1], (TILE, depth)) for v in xa), few)
                for t in range(2)
            ]
            real = jnp.concatenate([parts[0][0], parts[1][0]], axis=0)
            imag = jnp.concatenate([parts[0][1], parts[1][1]], axis=0)
            store_stacked(table, k * 2 * FR + a * TILE, FR, depth, real, imag)


def multiply(table, right, n, piece):
    value = right[:, :, n : n + piece]
    value = value.reshape(value.shape[0] * value.shape[1], piece)
    return jnp.dot(table[...], value, preferred_element_type=jnp.float32)


def given_kernel(slots, scale, *refs):
    sources, col, count, vis, out, kept, small = refs[:2], *refs[2:8]
    targets, table, small_sems, vis_sems = refs[8:10], *refs[10:]
    _, depth, width = vis.shape
    piece = width // vis_sems.shape[0]
    loads = small_copies(sources, targets, small_sems)
    blocks = [
        pltpu.make_async_copy(
            vis.at[:, :, pl.ds(n * piece, piece)], kept.at[:, :, pl.ds(n * piece, piece)], vis_sems.at[n]
        )
        for n in range(width // piece)
    ]
    for copy in loads + blocks:
        copy.start()
    for copy in loads:
        copy.wait()
    offs, order = targets
    c = lax.axis_index("col")
    u = col[0] + iota((TILE, depth), 1)
    sub = iota((TILE, depth), 0)
    small[0], small[1] = cis(u * sub)
    small[2], small[3] = cis(u * (sub * TILE))
    live = jnp.where(iota((TILE, depth), 1) < count[0, 0], scale, 0.0)
    starts = []
    for flip in (1, 0):
        for k in range(slots):
            slot = (((c // 2) ^ k) * 2) + ((c % 2) ^ flip)
            starts.append((offs[0, order[slot]] + (FS // 2 - FR // 2)) % NG)
    for k in range(0, 2 * slots, TILE):
        xs = cis(u * stacked_rows(starts[k : k + TILE], TILE))
        at = 4 + 2 * (k // TILE)
        small[at], small[at + 1] = xs[0] * live, xs[1] * live
    build_table(table, small, 0, slots, depth)
    for n in range(width // piece):
        blocks[n].wait()
        out[:, n * piece : (n + 1) * piece] = multiply(table, kept, n * piece, piece).astype(out.dtype)


def given_columns(slots, scale, offs, order, col, count, vis):
    _, depth, width = vis.shape
    rows = slots * 2 * FR
    smalls = 4 + 2 * -(-2 * slots // TILE)
    return pl.pallas_call(
        functools.partial(given_kernel, slots, scale),
        in_specs=[HBM] * 2 + [SMEM] * 2 + [HBM],
        out_specs=[VMEM] * 3,
        out_shape=[
            jax.ShapeDtypeStruct((rows, width), jnp.bfloat16),
            jax.ShapeDtypeStruct(vis.shape, vis.dtype),
            jax.ShapeDtypeStruct((smalls, TILE, depth), jnp.float32),
        ],
        scratch_shapes=[pltpu.SMEM(x.shape, x.dtype) for x in (offs, order)]
        + [
            pltpu.VMEM((rows, 2 * depth), jnp.bfloat16),
            pltpu.SemaphoreType.DMA((2,)),
            pltpu.SemaphoreType.DMA((4,)),
        ],
        compiler_params=pltpu.CompilerParams(vmem_limit_bytes=16 * MIB),
        cost_estimate=pl.CostEstimate(
            flops=rows * 4 * depth * width, bytes_accessed=4 * depth * width, transcendentals=0
        ),
        name="given",
    )(*in_hbm(offs, order), col, count, *in_hbm(vis))


def mine_kernel(slots, kept, small, out, table):
    _, depth, width = kept.shape
    build_table(table, small, slots, slots, depth)
    piece = 2 * LANES
    for n in range(0, width, piece):
        out[:, n : n + piece] = multiply(table, kept, n, piece)


def mine_columns(slots, kept, small):
    _, depth, width = kept.shape
    rows = slots * 2 * FR
    return pl.pallas_call(
        functools.partial(mine_kernel, slots),
        in_specs=[VMEM] * 2,
        out_specs=VMEM,
        out_shape=jax.ShapeDtypeStruct((rows, width), jnp.float32),
        scratch_shapes=[pltpu.VMEM((rows, 2 * depth), jnp.bfloat16)],
        compiler_params=pltpu.CompilerParams(vmem_limit_bytes=16 * MIB),
        cost_estimate=pl.CostEstimate(
            flops=rows * 4 * depth * width, bytes_accessed=4 * depth * width, transcendentals=0
        ),
        name="mine",
    )(kept, small)


def pair_kernel(mine, taken, total, *sent):
    high = total.shape[0]
    total[...] = mine[:high] + taken[:high].astype(jnp.float32)
    for k, out in enumerate(sent):
        at = slice((k + 1) * high, (k + 2) * high)
        out[...] = (mine[at] + taken[at].astype(jnp.float32)).astype(out.dtype)


def pair_sum(slots, mine, taken):
    rows, width = mine.shape
    high = rows // slots
    return pl.pallas_call(
        pair_kernel,
        in_specs=[VMEM] * 2,
        out_specs=[VMEM] * slots,
        out_shape=[jax.ShapeDtypeStruct((high, width), jnp.float32)]
        + [jax.ShapeDtypeStruct((high, width), jnp.bfloat16)] * (slots - 1),
        compiler_params=pltpu.CompilerParams(vmem_limit_bytes=8 * MIB),
        name="pair",
    )(mine, taken)


def sum_kernel(arrived, total, *refs):
    taken, outs = refs[:arrived], refs[arrived + 1 :]
    double, depth = outs[0].shape
    high = double // 2
    rows = len(outs)
    r = lax.axis_index("row")

    def rows_at(at):
        value = total[at, :]
        for other in taken:
            value = value + other[at, :].astype(jnp.float32)
        return value

    for p in range(rows):
        for z in range(2):
            if high % (2 * TILE) == 0:
                at = pl.ds(pl.multiple_of(z * FR + (r ^ p) * high, high), high)
                outs[p][z * high : (z + 1) * high, :] = rows_at(at).astype(outs[p].dtype)
    if high % (2 * TILE) != 0:
        value = rows_at(slice(0, 2 * FR))
        for p in range(rows):
            parts = []
            for z in range(2):
                part = value[z * FR : z * FR + high]
                for q in range(1, rows):
                    part = jnp.where((r ^ p) == q, value[z * FR + q * high : z * FR + (q + 1) * high], part)
                parts.append(part)
            outs[p][...] = jnp.concatenate(parts, axis=0).astype(outs[p].dtype)


def sum_of(rows, total, taken, wave):
    depth = total.shape[1]
    return pl.pallas_call(
        functools.partial(sum_kernel, len(taken)),
        in_specs=[VMEM] * (len(taken) + 1) + [HBM],
        out_specs=[VMEM] * rows,
        out_shape=[jax.ShapeDtypeStruct((2 * FR // rows, depth), jnp.bfloat16)] * rows,
        compiler_params=pltpu.CompilerParams(vmem_limit_bytes=16 * MIB),
        name="sum",
    )(total, *taken, wave)


def wave_kernel(rows, scale, after, *refs):
    del after
    sources, (out, turned, later) = refs[:3], refs[3:6]
    targets, sems = refs[6:9], refs[9]
    loads = small_copies(sources, targets, sems)
    for copy in loads:
        copy.start()
    depth, width = out.shape[0] // 2, out.shape[1]
    lane = iota((TILE, width), 1)
    sub = iota((TILE, width), 0)
    few = cis(lane * sub)

    def body(block, carry):
        coarse = cis(lane * ((block * TILE + sub) * TILE))
        base = block * (TILE * TILE)
        for a in range(0, TILE, 2):
            parts = [
                times(tuple(jnp.broadcast_to(v[a + s : a + s + 1], (TILE, width)) for v in coarse), few)
                for s in range(2)
            ]
            row = pl.multiple_of(base + a * TILE, 2 * TILE)
            for z in range(2):
                value = jnp.concatenate([parts[0][z], parts[1][z]], axis=0)
                out[pl.ds(row + z * depth, 2 * TILE), :] = value.astype(out.dtype)
        return carry

    lax.fori_loop(0, depth // (TILE * TILE), body, 0)
    for copy in loads:
        copy.wait()
    offs, order, roff = targets
    r = lax.axis_index("row")
    start = offs[1, order[lax.axis_index("col")]]
    height = later.shape[1]
    blocks = stacked_rows([(start + (r ^ b) * width) % NG for b in range(rows)], height)
    origins = [roff[r ^ p] for p in range(rows)]
    for p in range(rows):
        phase = cis((origins[p] + iota((height, depth), 1)) * blocks)
        turned[2 * p], turned[2 * p + 1] = phase[0] * scale, phase[1] * scale
    later[0], later[1] = cis(iota((height, width), 1) * stacked_rows(origins, height))
    j = ((r * width) + iota((height, width), 1)).astype(jnp.float32)
    for b in range(rows):
        j = ((r ^ b) * width + iota((1, width), 1)).astype(jnp.float32)
        later[2, b : b + 1, :] = 1.0 / (1.0 - BEAM_SLOPE * (j + 0.5) / FS)


def waves(rows, scale, offs, order, roff, after, depth, width):
    height = -(-rows // TILE) * TILE
    return pl.pallas_call(
        functools.partial(wave_kernel, rows, scale),
        in_specs=[HBM] * 4,
        out_specs=[VMEM] * 3,
        out_shape=[
            jax.ShapeDtypeStruct((2 * depth, width), jnp.bfloat16),
            jax.ShapeDtypeStruct((2 * rows, height, depth), jnp.float32),
            jax.ShapeDtypeStruct((3, height, width), jnp.float32),
        ],
        scratch_shapes=[pltpu.SMEM(x.shape, x.dtype) for x in (offs, order, roff)]
        + [pltpu.SemaphoreType.DMA((3,))],
        compiler_params=pltpu.CompilerParams(vmem_limit_bytes=16 * MIB),
        cost_estimate=pl.CostEstimate(flops=4 * 10**9, bytes_accessed=4 * depth * width, transcendentals=0),
        name="waves",
    )(after, *in_hbm(offs, order, roff))


def row_kernel(rows, wave, turned, later, *refs):
    pieces, outs, left = refs[:rows], refs[rows : 2 * rows], refs[2 * rows]
    double, depth = pieces[0].shape
    high = double // 2
    width = wave.shape[1]
    for p in range(rows):
        value = pieces[p][...].astype(jnp.float32)
        value = (value[:high], value[high:])
        for b in range(rows):
            turn = tuple(jnp.broadcast_to(turned[2 * p + z, b : b + 1, :], (high, depth)) for z in range(2))
            real, imag = times(value, turn)
            store_stacked(left, (p * rows + b) * double, high, depth, real, imag)
    piece = min(2 * LANES, width)
    largest = jnp.zeros((high, LANES), jnp.float32)
    for n in range(0, width, piece):
        product = jnp.dot(left[...], wave[:, n : n + piece], preferred_element_type=jnp.float32)
        for b in range(rows):
            real = imag = None
            for p in range(rows):
                at = (p * rows + b) * double
                value = (product[at : at + high], product[at + high : at + double])
                turn = tuple(later[z, p : p + 1, n : n + piece] for z in range(2))
                x, y = times(value, turn)
                real = x if real is None else real + x
                imag = y if imag is None else imag + y
            beam = later[2, b : b + 1, n : n + piece]
            real = real * beam
            imag = imag * beam
            power = real * real + imag * imag
            for m in range(0, piece, LANES):
                at = (n + m) // LANES * double
                outs[b][at : at + high] = real[:, m : m + LANES].astype(jnp.bfloat16)
                outs[b][at + high : at + double] = imag[:, m : m + LANES].astype(jnp.bfloat16)
                largest = jnp.maximum(largest, power[:, m : m + LANES])
    peak = jnp.broadcast_to(jnp.sqrt(jnp.max(largest, keepdims=True)), (2 * TILE, LANES))
    first = peak.astype(jnp.bfloat16).astype(jnp.float32)
    second = (peak - first).astype(jnp.bfloat16).astype(jnp.float32)
    third = peak - first - second
    sub = iota((2 * TILE, LANES), 0)
    peak = jnp.where(sub == 0, first, jnp.where(sub == 1, second, jnp.where(sub == 2, third, 0.0)))
    for b in range(rows):
        outs[b][width // LANES * double :] = peak.astype(jnp.bfloat16)


def rows_of(pieces, wave, turned, later):
    rows = len(pieces)
    double, depth = pieces[0].shape
    width = wave.shape[1]
    shape = jax.ShapeDtypeStruct((width // LANES * double + 2 * TILE, LANES), jnp.bfloat16)
    return pl.pallas_call(
        functools.partial(row_kernel, rows),
        in_specs=[VMEM] * (rows + 3),
        out_specs=[VMEM] * rows,
        out_shape=[shape] * rows,
        scratch_shapes=[pltpu.VMEM((rows * rows * double, 2 * depth), jnp.bfloat16)],
        compiler_params=pltpu.CompilerParams(vmem_limit_bytes=24 * MIB),
        cost_estimate=pl.CostEstimate(
            flops=rows * rows * double * 4 * depth * width, bytes_accessed=4 * depth * width, transcendentals=0
        ),
        name="rows",
    )(wave, turned, later, *pieces)


def finish_kernel(rows, *refs):
    pieces, (image, peak) = refs[:rows], refs[rows:]
    width = image.shape[3]
    high = image.shape[2] // rows
    r = lax.axis_index("row")
    largest = None
    for p in range(rows):
        for n in range(0, width, LANES):
            row = n // LANES * 2 * high
            if high % TILE == 0:
                at = pl.ds(pl.multiple_of((r ^ p) * high, high), high)
                value = pieces[p][row : row + 2 * high, :].astype(jnp.float32)
            else:
                at = pl.ds(p * high, high)
                value = pieces[0][row : row + 2 * high, :].astype(jnp.float32)
                for q in range(1, rows):
                    other = pieces[q][row : row + 2 * high, :].astype(jnp.float32)
                    value = jnp.where((r ^ p) == q, other, value)
            image[0, 0, at, n : n + LANES] = value[:high]
            image[0, 1, at, n : n + LANES] = value[high:]
        parts = pieces[p][width // LANES * 2 * high :, :].astype(jnp.float32)
        value = (parts[0:1] + parts[1:2]) + parts[2:3]
        largest = value if largest is None else jnp.maximum(largest, value)
    peak[0] = jnp.max(largest)


def finish(pieces, width):
    rows = len(pieces)
    return pl.pallas_call(
        functools.partial(finish_kernel, rows),
        in_specs=[VMEM] * rows,
        out_specs=[VMEM, SMEM],
        out_shape=[
            jax.ShapeDtypeStruct((1, 2, FR, width), jnp.float32),
            jax.ShapeDtypeStruct((1,), jnp.float32),
        ],
        compiler_params=pltpu.CompilerParams(vmem_limit_bytes=16 * MIB),
        name="finish",
    )(*pieces)


def local(visibilities, col_offsets, row_offsets, facet_offsets, facet_order, vis_counts):
    cols = lax.axis_size("col")
    rows = lax.axis_size("row")
    _, depth, width = visibilities.shape
    slots = cols // 2
    offsets = facet_offsets.T
    first_scale = 1.0 / math.sqrt(depth * cols)
    second_scale = 0.5 / math.sqrt(width * rows)

    def swap(value, axis, count, bit):
        return lax.ppermute(value, axis, [(i, i ^ bit) for i in range(count)])

    given, kept, small = given_columns(
        slots, first_scale, offsets, facet_order, col_offsets, vis_counts, visibilities
    )
    taken = swap(given, "col", cols, 1)
    mine = mine_columns(slots, kept, small)
    total, *sent = pair_sum(slots, mine, taken)
    sent = [swap(value, "col", cols, 2 * k + 2) for k, value in enumerate(sent)]
    wave, turned, later = waves(
        rows, second_scale, offsets, facet_order, row_offsets, total, width, FS // rows
    )
    pieces = sum_of(rows, total, sent, wave)
    pieces = [piece if p == 0 else swap(piece, "row", rows, p) for p, piece in enumerate(pieces)]
    parts = rows_of(pieces, wave, turned, later)
    parts = [part if p == 0 else swap(part, "row", rows, p) for p, part in enumerate(parts)]
    image, peak = finish(parts, FS // rows)
    return image, peak


def solution(mesh):
    in_specs = (P(None, "col", "row"), P("col"), P(), P(), P(), P("col", "row"))
    out_specs = (P("col", None, None, "row"), P("col"))
    return jax.shard_map(local, mesh=mesh, in_specs=in_specs, out_specs=out_specs, check_vma=False)
```

```python
import functools
import math

import jax
import jax.numpy as jnp
from jax import lax
from jax.experimental import pallas as pl
from jax.experimental.pallas import tpu as pltpu
from jax.sharding import PartitionSpec as P


FS = 4096
NG = 16384
FR = 64
BEAM_SLOPE = 0.66
LANES = 128
TILE = 8
MIB = 1 << 20
VMEM = pl.BlockSpec(memory_space=pltpu.VMEM)
SMEM = pl.BlockSpec(memory_space=pltpu.SMEM)
HBM = pl.BlockSpec(memory_space=pl.ANY)


def cis(phase):
    quarter = NG // 4
    turned = phase + quarter // 2
    quadrant = (turned & (NG - 1)) // quarter
    rest = (turned & (quarter - 1)) - quarter // 2
    t = rest.astype(jnp.float32) * (2.0 * math.pi / NG)
    t2 = t * t
    s = t * (1 + t2 * (-1 / 6 + t2 * (1 / 120 + t2 * (-1 / 5040 + t2 * (1 / 362880)))))
    c = 1 + t2 * (-1 / 2 + t2 * (1 / 24 + t2 * (-1 / 720 + t2 * (1 / 40320))))
    odd = (quadrant & 1) == 1
    real = jnp.where(odd, s, c)
    imag = jnp.where(odd, c, s)
    real = jnp.where((quadrant == 1) | (quadrant == 2), -real, real)
    imag = jnp.where(quadrant >= 2, -imag, imag)
    return real, imag


def times(a, b):
    return a[0] * b[0] - a[1] * b[1], a[0] * b[1] + a[1] * b[0]


def iota(shape, dim):
    return lax.broadcasted_iota(jnp.int32, shape, dim)


def stacked_rows(values, height):
    row = iota((height, 1), 0)
    result = jnp.zeros((height, 1), jnp.int32)
    for k, value in enumerate(values):
        result = jnp.where(row == k, value, result)
    return result


def store_stacked(ref, row, high, depth, real, imag):
    h = real.shape[0]
    real, imag, minus = (x.astype(jnp.bfloat16) for x in (real, imag, -imag))
    ref[row : row + h, :depth] = real
    ref[row : row + h, depth:] = minus
    ref[row + high : row + high + h, :depth] = imag
    ref[row + high : row + high + h, depth:] = real


def in_hbm(*arrays):
    return [pltpu.with_memory_space_constraint(x, pltpu.HBM) for x in arrays]


def small_copies(sources, targets, sems):
    return [pltpu.make_async_copy(s, t, sems.at[k]) for k, (s, t) in enumerate(zip(sources, targets))]


def build_table(table, small, first, slots, depth):
    few = (small[0], small[1])
    many = (small[2], small[3])
    for k in range(slots):
        k0, k1 = divmod(first + k, TILE)
        x = tuple(jnp.broadcast_to(small[4 + 2 * k0 + z, k1 : k1 + 1, :], (TILE, depth)) for z in range(2))
        xa = times(x, many)
        for a in range(0, FR // TILE, 2):
            parts = [
                times(tuple(jnp.broadcast_to(v[a + t : a + t + 1], (TILE, depth)) for v in xa), few)
                for t in range(2)
            ]
            real = jnp.concatenate([parts[0][0], parts[1][0]], axis=0)
            imag = jnp.concatenate([parts[0][1], parts[1][1]], axis=0)
            store_stacked(table, k * 2 * FR + a * TILE, FR, depth, real, imag)


def wave_rows(out, span, first, count, block):
    width = out.shape[1]
    lane = iota((TILE, width), 1)
    sub = iota((TILE, width), 0)
    few = cis(lane * sub)
    for k in range(count):
        base = (block * count + k) * (TILE * TILE)
        coarse = cis(lane * (first + base + sub * TILE))
        for a in range(0, TILE, 2):
            parts = [
                times(tuple(jnp.broadcast_to(v[a + t : a + t + 1], (TILE, width)) for v in coarse), few)
                for t in range(2)
            ]
            row = pl.multiple_of(base + a * TILE, 2 * TILE)
            for z in range(2):
                value = jnp.concatenate([parts[0][z], parts[1][z]], axis=0)
                out[pl.ds(row + z * span, 2 * TILE), :] = value.astype(out.dtype)


def multiply(table, right, first, out, beside=None):
    depth = right.shape[1]
    piece = 2 * LANES

    def step(n, carry):
        at = pl.ds(pl.multiple_of(n * piece, piece), piece)
        source = pl.ds(pl.multiple_of(first + n * piece, piece), piece)
        if beside is not None:
            beside(source, n)
        value = right[:, :, source].reshape(2 * depth, piece)
        out[:, at] = jnp.dot(table[...], value, preferred_element_type=jnp.float32).astype(out.dtype)
        return carry

    lax.fori_loop(0, out.shape[1] // piece, step, 0)


def first_kernel(slots, first_scale, second_scale, *refs):
    sources, (col, count, vis), outs = refs[:3], refs[3:6], refs[6:12]
    out, kept, other, own, turned, later = outs
    targets, (small, small_sems, vis_sems) = refs[12:15], refs[15:]
    _, depth, width = vis.shape
    piece = 2 * LANES
    loads = small_copies(sources, targets, small_sems)

    def block(at, n):
        return pltpu.make_async_copy(vis.at[:, :, at], kept.at[:, :, at], vis_sems.at[n])

    for copy in loads + [block(pl.ds(n * piece, piece), n) for n in range(width // piece)]:
        copy.start()
    for copy in loads:
        copy.wait()
    offs, order, roff = targets
    c = lax.axis_index("col")
    u = col[0] + iota((TILE, depth), 1)
    sub = iota((TILE, depth), 0)
    small[0], small[1] = cis(u * sub)
    small[2], small[3] = cis(u * (sub * TILE))
    live = jnp.where(iota((TILE, depth), 1) < count[0, 0], first_scale, 0.0)
    starts = []
    for flip in (1, 0):
        for k in range(slots):
            slot = (((c // 2) ^ k) * 2) + ((c % 2) ^ flip)
            starts.append((offs[0, order[slot]] + (FS // 2 - FR // 2)) % NG)
    for k in range(0, 2 * slots, TILE):
        xs = cis(u * stacked_rows(starts[k : k + TILE], TILE))
        at = 4 + 2 * (k // TILE)
        small[at], small[at + 1] = xs[0] * live, xs[1] * live
    build_table(other, small, 0, slots, depth)
    build_table(own, small, slots, slots, depth)
    rows = roff.shape[0]
    r = lax.axis_index("row")
    start = offs[1, order[c]]
    height, wide = later.shape[1:]
    blocks = stacked_rows([(start + (r ^ b) * wide) % NG for b in range(rows)], height)
    origins = [roff[r ^ p] for p in range(rows)]
    for p in range(rows):
        phase = cis((origins[p] + iota((height, width), 1)) * blocks)
        turned[2 * p], turned[2 * p + 1] = phase[0] * second_scale, phase[1] * second_scale
    later[0], later[1] = cis(iota((height, wide), 1) * stacked_rows(origins, height))
    for b in range(rows):
        j = ((r ^ b) * wide + iota((1, wide), 1)).astype(jnp.float32)
        later[2, b : b + 1, :] = 1.0 / (1.0 - BEAM_SLOPE * (j + 0.5) / FS)
    multiply(other, kept, 0, out, lambda at, n: block(at, n).wait())
    for n in range(out.shape[1] // piece, width // piece):
        block(pl.ds(n * piece, piece), n).wait()


def first_columns(slots, span, scales, wide, offs, order, roff, col, count, vis):
    _, depth, width = vis.shape
    tall = slots * 2 * FR
    rows = roff.shape[0]
    height = -(-rows // TILE) * TILE
    smalls = 4 + 2 * -(-2 * slots // TILE)
    return pl.pallas_call(
        functools.partial(first_kernel, slots, *scales),
        in_specs=[HBM] * 3 + [SMEM] * 2 + [HBM],
        out_specs=[VMEM] * 6,
        out_shape=[
            jax.ShapeDtypeStruct((tall, span), jnp.bfloat16),
            jax.ShapeDtypeStruct(vis.shape, vis.dtype),
            jax.ShapeDtypeStruct((tall, 2 * depth), jnp.bfloat16),
            jax.ShapeDtypeStruct((tall, 2 * depth), jnp.bfloat16),
            jax.ShapeDtypeStruct((2 * rows, height, width), jnp.float32),
            jax.ShapeDtypeStruct((3, height, wide), jnp.float32),
        ],
        scratch_shapes=[pltpu.SMEM(x.shape, x.dtype) for x in (offs, order, roff)]
        + [
            pltpu.VMEM((smalls, TILE, depth), jnp.float32),
            pltpu.SemaphoreType.DMA((3,)),
            pltpu.SemaphoreType.DMA((width // (2 * LANES),)),
        ],
        compiler_params=pltpu.CompilerParams(vmem_limit_bytes=20 * MIB),
        cost_estimate=pl.CostEstimate(flops=tall * 4 * depth * span, bytes_accessed=4 * depth * width, transcendentals=0),
        name="first",
    )(*in_hbm(offs, order, roff), col, count, *in_hbm(vis))


def more_kernel(first, waves, table, kept, after, out, *wave):
    del after
    span = out.shape[1]
    steps = span // (2 * LANES)

    def beside(source, n):
        if waves:
            wave_rows(wave[0], span, first, span // (steps * TILE * TILE), n)

    multiply(table, kept, first, out, beside)


def more_columns(first, span, dtype, wide, table, kept, after):
    _, depth, _ = kept.shape
    tall = table.shape[0]
    shape = [jax.ShapeDtypeStruct((tall, span), dtype)]
    if wide:
        shape.append(jax.ShapeDtypeStruct((2 * span, wide), jnp.bfloat16))
    return pl.pallas_call(
        functools.partial(more_kernel, first, bool(wide)),
        in_specs=[VMEM] * 2 + [HBM],
        out_specs=[VMEM] * len(shape),
        out_shape=shape,
        compiler_params=pltpu.CompilerParams(vmem_limit_bytes=16 * MIB),
        cost_estimate=pl.CostEstimate(flops=tall * 4 * depth * span, bytes_accessed=4 * depth * span, transcendentals=0),
        name="more",
    )(table, kept, after)


def pair_kernel(mine, taken, total, *sent):
    high = total.shape[0]
    total[...] = mine[:high] + taken[:high].astype(jnp.float32)
    for k, out in enumerate(sent):
        at = slice((k + 1) * high, (k + 2) * high)
        out[...] = (mine[at] + taken[at].astype(jnp.float32)).astype(out.dtype)


def pair_sum(slots, mine, taken):
    rows, width = mine.shape
    high = rows // slots
    return pl.pallas_call(
        pair_kernel,
        in_specs=[VMEM] * 2,
        out_specs=[VMEM] * slots,
        out_shape=[jax.ShapeDtypeStruct((high, width), jnp.float32)]
        + [jax.ShapeDtypeStruct((high, width), jnp.bfloat16)] * (slots - 1),
        compiler_params=pltpu.CompilerParams(vmem_limit_bytes=8 * MIB),
        name="pair",
    )(mine, taken)


def sum_kernel(arrived, total, *refs):
    taken, outs = refs[:arrived], refs[arrived:]
    double, _ = outs[0].shape
    high = double // 2
    rows = len(outs)
    span = high * rows
    r = lax.axis_index("row")

    def rows_at(at):
        value = total[at, :]
        for other in taken:
            value = value + other[at, :].astype(jnp.float32)
        return value

    for p in range(rows):
        for z in range(2):
            if high % TILE == 0:
                at = pl.ds(pl.multiple_of(z * span + (r ^ p) * high, high), high)
                outs[p][z * high : (z + 1) * high, :] = rows_at(at).astype(outs[p].dtype)
    if high % TILE != 0:
        value = rows_at(slice(0, 2 * span))
        for p in range(rows):
            parts = []
            for z in range(2):
                part = value[z * span : z * span + high]
                for q in range(1, rows):
                    at = z * span + q * high
                    part = jnp.where((r ^ p) == q, value[at : at + high], part)
                parts.append(part)
            outs[p][...] = jnp.concatenate(parts, axis=0).astype(outs[p].dtype)


def sum_of(rows, total, taken):
    depth = total.shape[1]
    return pl.pallas_call(
        functools.partial(sum_kernel, len(taken)),
        in_specs=[VMEM] * (len(taken) + 1),
        out_specs=[VMEM] * rows,
        out_shape=[jax.ShapeDtypeStruct((total.shape[0] // rows, depth), jnp.bfloat16)] * rows,
        compiler_params=pltpu.CompilerParams(vmem_limit_bytes=16 * MIB),
        name="sum",
    )(total, *taken)


def row_kernel(rows, first, earlier, last, wave, turned, later, *refs):
    pieces, refs = refs[:rows], refs[rows:]
    before, refs = refs[:earlier], refs[earlier:]
    outs, left = refs[:-1], refs[-1]
    double, span = pieces[0].shape
    high = double // 2
    width = wave.shape[1]
    for p in range(rows):
        value = pieces[p][...].astype(jnp.float32)
        value = (value[:high], value[high:])
        for b in range(rows):
            turn = tuple(
                jnp.broadcast_to(turned[2 * p + z, b : b + 1, first : first + span], (high, span)) for z in range(2)
            )
            real, imag = times(value, turn)
            store_stacked(left, (p * rows + b) * double, high, span, real, imag)
    piece = min(2 * LANES, width)
    largest = jnp.zeros((high, LANES), jnp.float32)
    for n in range(0, width, piece):
        product = jnp.dot(left[...], wave[:, n : n + piece], preferred_element_type=jnp.float32)
        if earlier:
            product = product + before[0][:, n : n + piece]
        if not last:
            outs[0][:, n : n + piece] = product
            continue
        for b in range(rows):
            real = imag = None
            for p in range(rows):
                at = (p * rows + b) * double
                value = (product[at : at + high], product[at + high : at + double])
                turn = tuple(later[z, p : p + 1, n : n + piece] for z in range(2))
                x, y = times(value, turn)
                real = x if real is None else real + x
                imag = y if imag is None else imag + y
            beam = later[2, b : b + 1, n : n + piece]
            real = real * beam
            imag = imag * beam
            power = real * real + imag * imag
            both = jnp.concatenate([real, imag], axis=0).astype(jnp.bfloat16)
            for m in range(0, piece, LANES):
                at = (n + m) // LANES * double
                outs[b][at : at + double] = both[:, m : m + LANES]
                largest = jnp.maximum(largest, power[:, m : m + LANES])
    if not last:
        return
    peak = jnp.broadcast_to(jnp.sqrt(jnp.max(largest, keepdims=True)), (2 * TILE, LANES))
    one = peak.astype(jnp.bfloat16).astype(jnp.float32)
    two = (peak - one).astype(jnp.bfloat16).astype(jnp.float32)
    three = peak - one - two
    sub = iota((2 * TILE, LANES), 0)
    peak = jnp.where(sub == 0, one, jnp.where(sub == 1, two, jnp.where(sub == 2, three, 0.0)))
    for b in range(rows):
        outs[b][width // LANES * double :] = peak.astype(jnp.bfloat16)


def rows_of(first, last, pieces, wave, turned, later, before):
    rows = len(pieces)
    double, span = pieces[0].shape
    width = wave.shape[1]
    if last:
        shape = [jax.ShapeDtypeStruct((width // LANES * double + 2 * TILE, LANES), jnp.bfloat16)] * rows
    else:
        shape = [jax.ShapeDtypeStruct((rows * rows * double, width), jnp.float32)]
    return pl.pallas_call(
        functools.partial(row_kernel, rows, first, len(before), last),
        in_specs=[VMEM] * (rows + 3 + len(before)),
        out_specs=[VMEM] * len(shape),
        out_shape=shape,
        scratch_shapes=[pltpu.VMEM((rows * rows * double, 2 * span), jnp.bfloat16)],
        compiler_params=pltpu.CompilerParams(vmem_limit_bytes=24 * MIB),
        cost_estimate=pl.CostEstimate(
            flops=rows * rows * double * 4 * span * width, bytes_accessed=4 * span * width, transcendentals=0
        ),
    )(wave, turned, later, *pieces, *before)


def finish_kernel(rows, chunks, *refs):
    pieces, (image, peak) = refs[:rows], refs[rows:]
    width = image.shape[3]
    high = image.shape[2] // (rows * chunks)
    tall = width // LANES * 2 * high
    r = lax.axis_index("row")
    largest = None
    for p in range(rows):
        for h in range(chunks):
            for n in range(0, width, LANES):
                row = h * tall + n // LANES * 2 * high
                if high % TILE == 0:
                    at = pl.ds(pl.multiple_of((h * rows + (r ^ p)) * high, high), high)
                    value = pieces[p][row : row + 2 * high, :].astype(jnp.float32)
                else:
                    at = pl.ds((h * rows + p) * high, high)
                    value = pieces[0][row : row + 2 * high, :].astype(jnp.float32)
                    for q in range(1, rows):
                        other = pieces[q][row : row + 2 * high, :].astype(jnp.float32)
                        value = jnp.where((r ^ p) == q, other, value)
                image[0, 0, at, n : n + LANES] = value[:high]
                image[0, 1, at, n : n + LANES] = value[high:]
        parts = pieces[p][chunks * tall :, :].astype(jnp.float32)
        value = (parts[0:1] + parts[1:2]) + parts[2:3]
        largest = value if largest is None else jnp.maximum(largest, value)
    peak[0] = jnp.max(largest)


def finish(pieces, chunks, width):
    rows = len(pieces)
    return pl.pallas_call(
        functools.partial(finish_kernel, rows, chunks),
        in_specs=[VMEM] * rows,
        out_specs=[VMEM, SMEM],
        out_shape=[
            jax.ShapeDtypeStruct((1, 2, FR, width), jnp.float32),
            jax.ShapeDtypeStruct((1,), jnp.float32),
        ],
        compiler_params=pltpu.CompilerParams(vmem_limit_bytes=16 * MIB),
        name="finish",
    )(*pieces)


def step(visibilities, col_offsets, row_offsets, facet_offsets, facet_order, vis_counts):
    cols = lax.axis_size("col")
    rows = lax.axis_size("row")
    _, depth, width = visibilities.shape
    slots = cols // 2
    wide = FS // rows
    chunks = 2
    span = width // chunks
    scales = (1.0 / math.sqrt(depth * cols), 0.5 / math.sqrt(width * rows))

    def swap(value, axis, count, bit):
        return lax.ppermute(value, axis, [(i, i ^ bit) for i in range(count)])

    given, kept, other, own, turned, later = first_columns(
        slots, span, scales, wide, facet_offsets.T, facet_order, row_offsets, col_offsets, vis_counts, visibilities
    )
    totals, sents, waves = [], [], []
    for h in range(chunks):
        if h > 0:
            (given,) = more_columns(h * span, span, jnp.bfloat16, 0, other, kept, totals[h - 1])
        taken = swap(given, "col", cols, 1)
        mine, wave = more_columns(h * span, span, jnp.float32, wide, own, kept, given)
        total, *sent = pair_sum(slots, mine, taken)
        waves.append(wave)
        totals.append(total)
        sents.append([swap(value, "col", cols, 2 * k + 2) for k, value in enumerate(sent)])
    pieces = []
    for h in range(chunks):
        mine, *others = sum_of(rows, totals[h], sents[h])
        far = [swap(value, "row", rows, p + 1) for p, value in reversed(list(enumerate(others)))]
        pieces.append([mine] + far[::-1])
    parts = []
    for h in range(chunks):
        parts = rows_of(h * span, h == chunks - 1, pieces[h], waves[h], turned, later, parts)
    far = [swap(part, "row", rows, p) for p, part in reversed(list(enumerate(parts))) if p > 0]
    parts = [parts[0]] + far[::-1]
    return tuple(finish(parts, 1, wide))


def solution(mesh):
    in_specs = (P(None, "col", "row"), P("col"), P(), P(), P(), P("col", "row"))
    out_specs = (P("col", None, None, "row"), P("col"))
    return jax.shard_map(step, mesh=mesh, in_specs=in_specs, out_specs=out_specs, check_vma=False)
```

```python
import functools
import math

import jax
import jax.numpy as jnp
from jax import lax
from jax.experimental import pallas as pl
from jax.experimental.pallas import tpu as pltpu
from jax.sharding import PartitionSpec as P


FS = 4096
NG = 16384
FR = 64
BEAM_SLOPE = 0.66
LANES = 128
TILE = 8
MIB = 1 << 20
VMEM = pl.BlockSpec(memory_space=pltpu.VMEM)
SMEM = pl.BlockSpec(memory_space=pltpu.SMEM)
HBM = pl.BlockSpec(memory_space=pl.ANY)


def cis(phase, period=NG):
    quarter = period // 4
    turned = phase + quarter // 2
    quadrant = (turned & (period - 1)) // quarter
    rest = (turned & (quarter - 1)) - quarter // 2
    t = rest.astype(jnp.float32) * (2.0 * math.pi / period)
    t2 = t * t
    s = t * (1 + t2 * (-1 / 6 + t2 * (1 / 120 + t2 * (-1 / 5040 + t2 * (1 / 362880)))))
    c = 1 + t2 * (-1 / 2 + t2 * (1 / 24 + t2 * (-1 / 720 + t2 * (1 / 40320))))
    odd = (quadrant & 1) == 1
    real = jnp.where(odd, s, c)
    imag = jnp.where(odd, c, s)
    real = jnp.where((quadrant == 1) | (quadrant == 2), -real, real)
    imag = jnp.where(quadrant >= 2, -imag, imag)
    return real, imag


def times(a, b):
    return a[0] * b[0] - a[1] * b[1], a[0] * b[1] + a[1] * b[0]


def iota(shape, dim):
    return lax.broadcasted_iota(jnp.int32, shape, dim)


def stacked_rows(values, height):
    row = iota((height, 1), 0)
    result = jnp.zeros((height, 1), jnp.int32)
    for k, value in enumerate(values):
        result = jnp.where(row == k, value, result)
    return result


def store_stacked(ref, row, high, depth, real, imag):
    h = real.shape[0]
    real, imag, minus = (x.astype(jnp.bfloat16) for x in (real, imag, -imag))
    ref[row : row + h, :depth] = real
    ref[row : row + h, depth:] = minus
    ref[row + high : row + high + h, :depth] = imag
    ref[row + high : row + high + h, depth:] = real


def in_hbm(*arrays):
    return [pltpu.with_memory_space_constraint(x, pltpu.HBM) for x in arrays]


def small_copies(sources, targets, sems):
    return [pltpu.make_async_copy(s, t, sems.at[k]) for k, (s, t) in enumerate(zip(sources, targets))]


def build_table(table, small, first, slots, depth):
    few = (small[0], small[1])
    many = (small[2], small[3])
    for k in range(slots):
        k0, k1 = divmod(first + k, TILE)
        x = tuple(jnp.broadcast_to(small[4 + 2 * k0 + z, k1 : k1 + 1, :], (TILE, depth)) for z in range(2))
        xa = times(x, many)
        for a in range(0, FR // TILE, 2):
            parts = [
                times(tuple(jnp.broadcast_to(v[a + t : a + t + 1], (TILE, depth)) for v in xa), few)
                for t in range(2)
            ]
            real = jnp.concatenate([parts[0][0], parts[1][0]], axis=0)
            imag = jnp.concatenate([parts[0][1], parts[1][1]], axis=0)
            store_stacked(table, k * 2 * FR + a * TILE, FR, depth, real, imag)


def wave_rows(out, start):
    half, width = out.shape[0] // 2, out.shape[1]
    lane = iota((TILE, width), 1)
    sub = iota((TILE, width), 0)
    few = cis(lane * sub)
    coarse = cis(lane * (start + sub * (2 * TILE)), 2 * NG)
    stride = cis(lane * (TILE * TILE))
    for base in range(0, half, TILE * TILE):
        if base > 0:
            coarse = times(coarse, stride)
        for a in range(0, TILE, 2):
            parts = [
                times(tuple(jnp.broadcast_to(v[a + t : a + t + 1], (TILE, width)) for v in coarse), few)
                for t in range(2)
            ]
            row = base + a * TILE
            for z in range(2):
                value = jnp.concatenate([parts[0][z], parts[1][z]], axis=0)
                out[row + z * half : row + z * half + 2 * TILE, :] = value.astype(out.dtype)


def blocks_of(chunk, half, width):
    return chunk * half, width - (chunk + 1) * half


def multiply(table, right, chunk, out):
    depth, width = right.shape[1:]
    half = out.shape[1] // 2
    for k, start in enumerate(blocks_of(chunk, half, width)):
        value = right[:, :, start : start + half].reshape(2 * depth, half)
        product = jnp.dot(table[...], value, preferred_element_type=jnp.float32)
        out[:, k * half : (k + 1) * half] = product.astype(out.dtype)


def first_kernel(slots, first_scale, second_scale, *refs):
    sources, (col, count, vis), outs = refs[:3], refs[3:6], refs[6:12]
    out, kept, other, own, turned, later = outs
    targets, (small, small_sems, vis_sems) = refs[12:15], refs[15:]
    _, depth, width = vis.shape
    half = out.shape[1] // 2
    loads = small_copies(sources, targets, small_sems)

    def block(start, n):
        at = pl.ds(start, half)
        return pltpu.make_async_copy(vis.at[:, :, at], kept.at[:, :, at], vis_sems.at[n])

    def wait(n, carry):
        block(0, n).wait()
        return carry

    order_of_blocks = [start for h in range(width // (2 * half)) for start in blocks_of(h, half, width)]
    for copy in loads + [block(start, n) for n, start in enumerate(order_of_blocks)]:
        copy.start()
    for copy in loads:
        copy.wait()
    offs, order, roff = targets
    c = lax.axis_index("col")
    u = col[0] + iota((TILE, depth), 1)
    sub = iota((TILE, depth), 0)
    small[0], small[1] = cis(u * sub)
    small[2], small[3] = cis(u * (sub * TILE))
    live = jnp.where(iota((TILE, depth), 1) < count[0, 0], first_scale, 0.0)
    starts = []
    for flip in (1, 0):
        for k in range(slots):
            slot = (((c // 2) ^ k) * 2) + ((c % 2) ^ flip)
            starts.append((offs[0, order[slot]] + (FS // 2 - FR // 2)) % NG)
    for k in range(0, 2 * slots, TILE):
        xs = cis(u * stacked_rows(starts[k : k + TILE], TILE))
        at = 4 + 2 * (k // TILE)
        small[at], small[at + 1] = xs[0] * live, xs[1] * live
    build_table(other, small, 0, slots, depth)
    build_table(own, small, slots, slots, depth)
    rows = roff.shape[0]
    r = lax.axis_index("row")
    start = offs[1, order[c]]
    height, wide = later.shape[1:]
    blocks = stacked_rows([(start + (r ^ b) * wide) % NG for b in range(rows)], height)
    origins = [roff[r ^ p] for p in range(rows)]
    lane = iota((height, half), 1)
    for n, first in enumerate(order_of_blocks):
        v = first + (half - 1 - lane if n % 2 == 0 else lane)
        for p in range(rows):
            phase = cis((origins[p] + v) * blocks)
            for z in range(2):
                turned[2 * p + z, :, n * half : (n + 1) * half] = phase[z] * second_scale
    middle = [2 * origin + (width - 1) for origin in origins]
    later[0], later[1] = cis(iota((height, wide), 1) * stacked_rows(middle, height), 2 * NG)
    for b in range(rows):
        j = ((r ^ b) * wide + iota((1, wide), 1)).astype(jnp.float32)
        later[2, b : b + 1, :] = 1.0 / (1.0 - BEAM_SLOPE * (j + 0.5) / FS)
    lax.fori_loop(0, 2, wait, 0)
    multiply(other, kept, 0, out)
    lax.fori_loop(2, len(order_of_blocks), wait, 0)


def first_columns(slots, span, scales, wide, offs, order, roff, col, count, vis):
    _, depth, width = vis.shape
    tall = slots * 2 * FR
    rows = roff.shape[0]
    height = -(-rows // TILE) * TILE
    smalls = 4 + 2 * -(-2 * slots // TILE)
    return pl.pallas_call(
        functools.partial(first_kernel, slots, *scales),
        in_specs=[HBM] * 3 + [SMEM] * 2 + [HBM],
        out_specs=[VMEM] * 6,
        out_shape=[
            jax.ShapeDtypeStruct((tall, span), jnp.bfloat16),
            jax.ShapeDtypeStruct(vis.shape, vis.dtype),
            jax.ShapeDtypeStruct((tall, 2 * depth), jnp.bfloat16),
            jax.ShapeDtypeStruct((tall, 2 * depth), jnp.bfloat16),
            jax.ShapeDtypeStruct((2 * rows, height, width), jnp.float32),
            jax.ShapeDtypeStruct((3, height, wide), jnp.float32),
        ],
        scratch_shapes=[pltpu.SMEM(x.shape, x.dtype) for x in (offs, order, roff)]
        + [
            pltpu.VMEM((smalls, TILE, depth), jnp.float32),
            pltpu.SemaphoreType.DMA((3,)),
            pltpu.SemaphoreType.DMA((2 * width // span,)),
        ],
        compiler_params=pltpu.CompilerParams(vmem_limit_bytes=20 * MIB),
        cost_estimate=pl.CostEstimate(flops=tall * 4 * depth * span, bytes_accessed=4 * depth * width, transcendentals=0),
        name="first",
    )(*in_hbm(offs, order, roff), col, count, *in_hbm(vis))


def more_kernel(chunk, table, kept, after, out, *wave):
    del after
    if wave:
        width = kept.shape[2]
        wave_rows(wave[0], 2 * blocks_of(chunk, out.shape[1] // 2, width)[1] - (width - 1))
    multiply(table, kept, chunk, out)


def more_columns(chunk, span, dtype, wide, table, kept, after):
    _, depth, _ = kept.shape
    tall = table.shape[0]
    shape = [jax.ShapeDtypeStruct((tall, span), dtype)]
    if wide:
        shape.append(jax.ShapeDtypeStruct((span, wide), jnp.bfloat16))
    return pl.pallas_call(
        functools.partial(more_kernel, chunk),
        in_specs=[VMEM] * 2 + [HBM],
        out_specs=[VMEM] * len(shape),
        out_shape=shape,
        compiler_params=pltpu.CompilerParams(vmem_limit_bytes=16 * MIB),
        cost_estimate=pl.CostEstimate(flops=tall * 4 * depth * span, bytes_accessed=4 * depth * span, transcendentals=0),
        name="more",
    )(table, kept, after)


def pair_kernel(mine, taken, total, *sent):
    high = total.shape[0]
    total[...] = mine[:high] + taken[:high].astype(jnp.float32)
    for k, out in enumerate(sent):
        at = slice((k + 1) * high, (k + 2) * high)
        out[...] = (mine[at] + taken[at].astype(jnp.float32)).astype(out.dtype)


def pair_sum(slots, mine, taken):
    rows, width = mine.shape
    high = rows // slots
    return pl.pallas_call(
        pair_kernel,
        in_specs=[VMEM] * 2,
        out_specs=[VMEM] * slots,
        out_shape=[jax.ShapeDtypeStruct((high, width), jnp.float32)]
        + [jax.ShapeDtypeStruct((high, width), jnp.bfloat16)] * (slots - 1),
        compiler_params=pltpu.CompilerParams(vmem_limit_bytes=8 * MIB),
        name="pair",
    )(mine, taken)


def sum_kernel(arrived, total, *refs):
    taken, outs = refs[:arrived], refs[arrived:]
    double, _ = outs[0].shape
    high = double // 2
    rows = len(outs)
    span = high * rows
    r = lax.axis_index("row")

    def rows_at(at):
        value = total[at, :]
        for other in taken:
            value = value + other[at, :].astype(jnp.float32)
        return value

    for p in range(rows):
        for z in range(2):
            if high % TILE == 0:
                at = pl.ds(pl.multiple_of(z * span + (r ^ p) * high, high), high)
                outs[p][z * high : (z + 1) * high, :] = rows_at(at).astype(outs[p].dtype)
    if high % TILE != 0:
        value = rows_at(slice(0, 2 * span))
        for p in range(rows):
            parts = []
            for z in range(2):
                part = value[z * span : z * span + high]
                for q in range(1, rows):
                    at = z * span + q * high
                    part = jnp.where((r ^ p) == q, value[at : at + high], part)
                parts.append(part)
            outs[p][...] = jnp.concatenate(parts, axis=0).astype(outs[p].dtype)


def sum_of(rows, total, taken):
    depth = total.shape[1]
    return pl.pallas_call(
        functools.partial(sum_kernel, len(taken)),
        in_specs=[VMEM] * (len(taken) + 1),
        out_specs=[VMEM] * rows,
        out_shape=[jax.ShapeDtypeStruct((total.shape[0] // rows, depth), jnp.bfloat16)] * rows,
        compiler_params=pltpu.CompilerParams(vmem_limit_bytes=16 * MIB),
        name="sum",
    )(total, *taken)


def row_kernel(rows, first, earlier, last, wave, turned, later, *refs):
    pieces, refs = refs[:rows], refs[rows:]
    before, refs = refs[:earlier], refs[earlier:]
    outs, left = refs[:-1], refs[-1]
    double, span = pieces[0].shape
    high = double // 2
    width = wave.shape[1]
    half = span // 2
    mirror = jnp.where(iota((half, half), 0) + iota((half, half), 1) == half - 1, 1.0, 0.0).astype(jnp.bfloat16)
    firsts = jnp.concatenate([pieces[p][:, :half] for p in range(rows)], axis=0)
    firsts = jnp.dot(firsts, mirror, preferred_element_type=jnp.float32)
    for p in range(rows):
        near = firsts[p * double : (p + 1) * double]
        far = pieces[p][:, half:].astype(jnp.float32)
        for b in range(rows):

            def turn(value, at):
                factor = (turned[2 * p + z, b : b + 1, first + at : first + at + half] for z in range(2))
                factor = tuple(jnp.broadcast_to(v, (high, half)) for v in factor)
                return times((value[:high], value[high:]), factor)

            x, y = turn(near, 0), turn(far, half)
            even = (y[0] + x[0], y[1] + x[1])
            odd = (y[0] - x[0], y[1] - x[1])
            at = (p * rows + b) * double
            left[at : at + high, :half] = even[0].astype(left.dtype)
            left[at : at + high, half:] = (-odd[1]).astype(left.dtype)
            left[at + high : at + double, :half] = even[1].astype(left.dtype)
            left[at + high : at + double, half:] = odd[0].astype(left.dtype)
    piece = min(2 * LANES, width)
    largest = jnp.zeros((high, LANES), jnp.float32)
    for n in range(0, width, piece):
        product = jnp.dot(left[...], wave[:, n : n + piece], preferred_element_type=jnp.float32)
        if earlier:
            product = product + before[0][:, n : n + piece]
        if not last:
            outs[0][:, n : n + piece] = product
            continue
        for b in range(rows):
            real = imag = None
            for p in range(rows):
                at = (p * rows + b) * double
                value = (product[at : at + high], product[at + high : at + double])
                turn = tuple(later[z, p : p + 1, n : n + piece] for z in range(2))
                x, y = times(value, turn)
                real = x if real is None else real + x
                imag = y if imag is None else imag + y
            beam = later[2, b : b + 1, n : n + piece]
            real = real * beam
            imag = imag * beam
            power = real * real + imag * imag
            both = jnp.concatenate([real, imag], axis=0).astype(jnp.bfloat16)
            for m in range(0, piece, LANES):
                at = (n + m) // LANES * double
                outs[b][at : at + double] = both[:, m : m + LANES]
                largest = jnp.maximum(largest, power[:, m : m + LANES])
    if not last:
        return
    peak = jnp.broadcast_to(jnp.sqrt(jnp.max(largest, keepdims=True)), (2 * TILE, LANES))
    one = peak.astype(jnp.bfloat16).astype(jnp.float32)
    two = (peak - one).astype(jnp.bfloat16).astype(jnp.float32)
    three = peak - one - two
    sub = iota((2 * TILE, LANES), 0)
    peak = jnp.where(sub == 0, one, jnp.where(sub == 1, two, jnp.where(sub == 2, three, 0.0)))
    for b in range(rows):
        outs[b][width // LANES * double :] = peak.astype(jnp.bfloat16)


def rows_of(first, last, pieces, wave, turned, later, before):
    rows = len(pieces)
    double, span = pieces[0].shape
    width = wave.shape[1]
    if last:
        shape = [jax.ShapeDtypeStruct((width // LANES * double + 2 * TILE, LANES), jnp.bfloat16)] * rows
    else:
        shape = [jax.ShapeDtypeStruct((rows * rows * double, width), jnp.float32)]
    return pl.pallas_call(
        functools.partial(row_kernel, rows, first, len(before), last),
        in_specs=[VMEM] * (rows + 3 + len(before)),
        out_specs=[VMEM] * len(shape),
        out_shape=shape,
        scratch_shapes=[pltpu.VMEM((rows * rows * double, span), jnp.bfloat16)],
        compiler_params=pltpu.CompilerParams(vmem_limit_bytes=24 * MIB),
        cost_estimate=pl.CostEstimate(
            flops=rows * rows * double * 2 * span * width, bytes_accessed=2 * span * width, transcendentals=0
        ),
    )(wave, turned, later, *pieces, *before)


def finish_kernel(rows, chunks, *refs):
    pieces, (image, peak) = refs[:rows], refs[rows:]
    width = image.shape[3]
    high = image.shape[2] // (rows * chunks)
    tall = width // LANES * 2 * high
    r = lax.axis_index("row")
    largest = None
    for p in range(rows):
        for h in range(chunks):
            for n in range(0, width, LANES):
                row = h * tall + n // LANES * 2 * high
                if high % TILE == 0:
                    at = pl.ds(pl.multiple_of((h * rows + (r ^ p)) * high, high), high)
                    value = pieces[p][row : row + 2 * high, :].astype(jnp.float32)
                else:
                    at = pl.ds((h * rows + p) * high, high)
                    value = pieces[0][row : row + 2 * high, :].astype(jnp.float32)
                    for q in range(1, rows):
                        other = pieces[q][row : row + 2 * high, :].astype(jnp.float32)
                        value = jnp.where((r ^ p) == q, other, value)
                image[0, 0, at, n : n + LANES] = value[:high]
                image[0, 1, at, n : n + LANES] = value[high:]
        parts = pieces[p][chunks * tall :, :].astype(jnp.float32)
        value = (parts[0:1] + parts[1:2]) + parts[2:3]
        largest = value if largest is None else jnp.maximum(largest, value)
    peak[0] = jnp.max(largest)


def finish(pieces, chunks, width):
    rows = len(pieces)
    return pl.pallas_call(
        functools.partial(finish_kernel, rows, chunks),
        in_specs=[VMEM] * rows,
        out_specs=[VMEM, SMEM],
        out_shape=[
            jax.ShapeDtypeStruct((1, 2, FR, width), jnp.float32),
            jax.ShapeDtypeStruct((1,), jnp.float32),
        ],
        compiler_params=pltpu.CompilerParams(vmem_limit_bytes=16 * MIB),
        name="finish",
    )(*pieces)


def step(visibilities, col_offsets, row_offsets, facet_offsets, facet_order, vis_counts):
    cols = lax.axis_size("col")
    rows = lax.axis_size("row")
    _, depth, width = visibilities.shape
    slots = cols // 2
    wide = FS // rows
    chunks = 2
    span = width // chunks
    scales = (1.0 / math.sqrt(depth * cols), 0.5 / math.sqrt(width * rows))

    def swap(value, axis, count, bit):
        return lax.ppermute(value, axis, [(i, i ^ bit) for i in range(count)])

    given, kept, other, own, turned, later = first_columns(
        slots, span, scales, wide, facet_offsets.T, facet_order, row_offsets, col_offsets, vis_counts, visibilities
    )
    totals, sents, waves = [], [], []
    for h in range(chunks):
        if h > 0:
            (given,) = more_columns(h, span, jnp.bfloat16, 0, other, kept, totals[h - 1])
        taken = swap(given, "col", cols, 1)
        mine, wave = more_columns(h, span, jnp.float32, wide, own, kept, given)
        total, *sent = pair_sum(slots, mine, taken)
        waves.append(wave)
        totals.append(total)
        sents.append([swap(value, "col", cols, 2 * k + 2) for k, value in enumerate(sent)])
    pieces = []
    for h in range(chunks):
        mine, *others = sum_of(rows, totals[h], sents[h])
        far = [swap(value, "row", rows, p + 1) for p, value in reversed(list(enumerate(others)))]
        pieces.append([mine] + far[::-1])
    parts = []
    for h in range(chunks):
        parts = rows_of(h * span, h == chunks - 1, pieces[h], waves[h], turned, later, parts)
    far = [swap(part, "row", rows, p) for p, part in reversed(list(enumerate(parts))) if p > 0]
    parts = [parts[0]] + far[::-1]
    return tuple(finish(parts, 1, wide))


def solution(mesh):
    in_specs = (P(None, "col", "row"), P("col"), P(), P(), P(), P("col", "row"))
    out_specs = (P("col", None, None, "row"), P("col"))
    return jax.shard_map(step, mesh=mesh, in_specs=in_specs, out_specs=out_specs, check_vma=False)
```

```python
import functools
import math

import jax
import jax.numpy as jnp
from jax import lax
from jax.experimental import pallas as pl
from jax.experimental.pallas import tpu as pltpu
from jax.sharding import PartitionSpec as P


FS = 4096
NG = 16384
FR = 64
BEAM_SLOPE = 0.66
LANES = 128
TILE = 8
MIB = 1 << 20
VMEM = pl.BlockSpec(memory_space=pltpu.VMEM)
SMEM = pl.BlockSpec(memory_space=pltpu.SMEM)
HBM = pl.BlockSpec(memory_space=pl.ANY)


def cis(phase, period=NG):
    quarter = period // 4
    turned = phase + quarter // 2
    quadrant = (turned & (period - 1)) // quarter
    rest = (turned & (quarter - 1)) - quarter // 2
    t = rest.astype(jnp.float32) * (2.0 * math.pi / period)
    t2 = t * t
    s = t * (1 + t2 * (-1 / 6 + t2 * (1 / 120 + t2 * (-1 / 5040 + t2 * (1 / 362880)))))
    c = 1 + t2 * (-1 / 2 + t2 * (1 / 24 + t2 * (-1 / 720 + t2 * (1 / 40320))))
    odd = (quadrant & 1) == 1
    real = jnp.where(odd, s, c)
    imag = jnp.where(odd, c, s)
    real = jnp.where((quadrant == 1) | (quadrant == 2), -real, real)
    imag = jnp.where(quadrant >= 2, -imag, imag)
    return real, imag


def times(a, b):
    return a[0] * b[0] - a[1] * b[1], a[0] * b[1] + a[1] * b[0]


def iota(shape, dim):
    return lax.broadcasted_iota(jnp.int32, shape, dim)


def stacked_rows(values, height):
    row = iota((height, 1), 0)
    result = jnp.zeros((height, 1), jnp.int32)
    for k, value in enumerate(values):
        result = jnp.where(row == k, value, result)
    return result


def store_stacked(ref, row, high, depth, real, imag):
    h = real.shape[0]
    real, imag, minus = (x.astype(jnp.bfloat16) for x in (real, imag, -imag))
    ref[row : row + h, :depth] = real
    ref[row : row + h, depth:] = minus
    ref[row + high : row + high + h, :depth] = imag
    ref[row + high : row + high + h, depth:] = real


def in_hbm(*arrays):
    return [pltpu.with_memory_space_constraint(x, pltpu.HBM) for x in arrays]


def small_copies(sources, targets, sems):
    return [pltpu.make_async_copy(s, t, sems.at[k]) for k, (s, t) in enumerate(zip(sources, targets))]


def build_table(table, small, first, slots, depth):
    few = (small[0], small[1])
    many = (small[2], small[3])
    for k in range(slots):
        k0, k1 = divmod(first + k, TILE)
        x = tuple(jnp.broadcast_to(small[4 + 2 * k0 + z, k1 : k1 + 1, :], (TILE, depth)) for z in range(2))
        xa = times(x, many)
        for a in range(0, FR // TILE, 2):
            parts = [
                times(tuple(jnp.broadcast_to(v[a + t : a + t + 1], (TILE, depth)) for v in xa), few)
                for t in range(2)
            ]
            real = jnp.concatenate([parts[0][0], parts[1][0]], axis=0)
            imag = jnp.concatenate([parts[0][1], parts[1][1]], axis=0)
            store_stacked(table, k * 2 * FR + a * TILE, FR, depth, real, imag)


def wave_rows(out, start):
    half, width = out.shape[0] // 2, out.shape[1]
    lane = iota((TILE, width), 1)
    sub = iota((TILE, width), 0)
    few = cis(lane * sub)
    coarse = cis(lane * (start + sub * (2 * TILE)), 2 * NG)
    stride = cis(lane * (TILE * TILE))
    for base in range(0, half, TILE * TILE):
        if base > 0:
            coarse = times(coarse, stride)
        for a in range(0, TILE, 2):
            parts = [
                times(tuple(jnp.broadcast_to(v[a + t : a + t + 1], (TILE, width)) for v in coarse), few)
                for t in range(2)
            ]
            row = base + a * TILE
            for z in range(2):
                value = jnp.concatenate([parts[0][z], parts[1][z]], axis=0)
                out[row + z * half : row + z * half + 2 * TILE, :] = value.astype(out.dtype)


def blocks_of(chunk, half, width):
    return chunk * half, width - (chunk + 1) * half


def multiply(table, right, blocks, out):
    depth = right.shape[1]
    half = out.shape[1] // len(blocks)
    for k, start in enumerate(blocks):
        value = right[:, :, start : start + half].reshape(2 * depth, half)
        product = jnp.dot(table[...], value, preferred_element_type=jnp.float32)
        out[:, k * half : (k + 1) * half] = product.astype(out.dtype)


def mirrored_blocks(half, width):
    return [start for h in range(width // (2 * half)) for start in blocks_of(h, half, width)]


def first_kernel(slots, scale, *refs):
    sources, (col, count, vis), (out, kept, other, small) = refs[:2], refs[2:5], refs[5:9]
    targets, (small_sems, vis_sems) = refs[9:11], refs[11:]
    _, depth, width = vis.shape
    half = out.shape[1] // 2
    loads = small_copies(sources, targets, small_sems)
    starts = mirrored_blocks(half, width)

    def block(start, n):
        at = pl.ds(start, half)
        return pltpu.make_async_copy(vis.at[:, :, at], kept.at[:, :, at], vis_sems.at[n])

    def wait(n, carry):
        block(0, n).wait()
        return carry

    for copy in loads + [block(start, n) for n, start in enumerate(starts)]:
        copy.start()
    u = col[0] + iota((TILE, depth), 1)
    sub = iota((TILE, depth), 0)
    small[0], small[1] = cis(u * sub)
    small[2], small[3] = cis(u * (sub * TILE))
    c = lax.axis_index("col")

    @pl.when(c >= 0)
    def arrived():
        for copy in loads:
            copy.wait()

    offs, order = targets
    live = jnp.where(iota((TILE, depth), 1) < count[0, 0], scale, 0.0)
    origins = []
    for flip in (1, 0):
        for k in range(slots):
            slot = (((c // 2) ^ k) * 2) + ((c % 2) ^ flip)
            origins.append((offs[0, order[slot]] + (FS // 2 - FR // 2)) % NG)
    for k in range(0, 2 * slots, TILE):
        xs = cis(u * stacked_rows(origins[k : k + TILE], TILE))
        at = 4 + 2 * (k // TILE)
        small[at], small[at + 1] = xs[0] * live, xs[1] * live
    build_table(other, small, 0, slots, depth)
    lax.fori_loop(0, 2, wait, 0)
    multiply(other, kept, blocks_of(0, half, width), out)
    lax.fori_loop(2, len(starts), wait, 0)


def first_columns(slots, span, scale, offs, order, col, count, vis):
    _, depth, width = vis.shape
    tall = slots * 2 * FR
    smalls = 4 + 2 * -(-2 * slots // TILE)
    return pl.pallas_call(
        functools.partial(first_kernel, slots, scale),
        in_specs=[HBM] * 2 + [SMEM] * 2 + [HBM],
        out_specs=[VMEM] * 4,
        out_shape=[
            jax.ShapeDtypeStruct((tall, span), jnp.bfloat16),
            jax.ShapeDtypeStruct(vis.shape, vis.dtype),
            jax.ShapeDtypeStruct((tall, 2 * depth), jnp.bfloat16),
            jax.ShapeDtypeStruct((smalls, TILE, depth), jnp.float32),
        ],
        scratch_shapes=[pltpu.SMEM(x.shape, x.dtype) for x in (offs, order)]
        + [pltpu.SemaphoreType.DMA((2,)), pltpu.SemaphoreType.DMA((2 * width // span,))],
        compiler_params=pltpu.CompilerParams(vmem_limit_bytes=20 * MIB),
        cost_estimate=pl.CostEstimate(flops=tall * 4 * depth * span, bytes_accessed=4 * depth * width, transcendentals=0),
        name="first",
    )(*in_hbm(offs, order), col, count, *in_hbm(vis))


def more_kernel(blocks, table, kept, after, out):
    del after
    multiply(table, kept, blocks, out)


def more_columns(blocks, half, dtype, table, kept, after):
    depth = kept.shape[1]
    tall = table.shape[0]
    span = half * len(blocks)
    return pl.pallas_call(
        functools.partial(more_kernel, blocks),
        in_specs=[VMEM] * 2 + [HBM],
        out_specs=VMEM,
        out_shape=jax.ShapeDtypeStruct((tall, span), dtype),
        compiler_params=pltpu.CompilerParams(vmem_limit_bytes=16 * MIB),
        cost_estimate=pl.CostEstimate(flops=tall * 4 * depth * span, bytes_accessed=4 * depth * span, transcendentals=0),
        name="more",
    )(table, kept, after)


def own_kernel(slots, blocks, small, kept, after, out, table):
    del after
    build_table(table, small, slots, slots, kept.shape[1])
    multiply(table, kept, blocks, out)


def own_columns(slots, blocks, half, small, kept, after):
    depth = kept.shape[1]
    tall = slots * 2 * FR
    span = half * len(blocks)
    return pl.pallas_call(
        functools.partial(own_kernel, slots, blocks),
        in_specs=[VMEM] * 2 + [HBM],
        out_specs=[VMEM] * 2,
        out_shape=[
            jax.ShapeDtypeStruct((tall, span), jnp.float32),
            jax.ShapeDtypeStruct((tall, 2 * depth), jnp.bfloat16),
        ],
        compiler_params=pltpu.CompilerParams(vmem_limit_bytes=16 * MIB),
        cost_estimate=pl.CostEstimate(flops=tall * 4 * depth * span, bytes_accessed=4 * depth * span, transcendentals=0),
        name="own",
    )(small, kept, after)


def turn_kernel(scale, chunks, after, *refs):
    del after
    sources, refs = refs[:3], refs[3:]
    waves, (turned, later) = refs[:chunks], refs[chunks : chunks + 2]
    targets, sems = refs[chunks + 2 : chunks + 5], refs[chunks + 5]
    loads = small_copies(sources, targets, sems)
    for copy in loads:
        copy.start()
    width = turned.shape[2]
    half = width // (2 * chunks)
    for h in range(chunks):
        wave_rows(waves[h], 2 * blocks_of(h, half, width)[1] - (width - 1))

    @pl.when(lax.axis_index("col") >= 0)
    def arrived():
        for copy in loads:
            copy.wait()

    offs, order, roff = targets
    rows = roff.shape[0]
    r = lax.axis_index("row")
    start = offs[1, order[lax.axis_index("col")]]
    height, wide = later.shape[1:]
    blocks = stacked_rows([(start + (r ^ b) * wide) % NG for b in range(rows)], height)
    origins = [roff[r ^ p] for p in range(rows)]
    lane = iota((height, half), 1)
    for n, first in enumerate(mirrored_blocks(half, width)):
        v = first + (half - 1 - lane if n % 2 == 0 else lane)
        for p in range(rows):
            phase = cis((origins[p] + v) * blocks)
            for z in range(2):
                turned[2 * p + z, :, n * half : (n + 1) * half] = phase[z] * scale
    middle = [2 * origin + (width - 1) for origin in origins]
    later[0], later[1] = cis(iota((height, wide), 1) * stacked_rows(middle, height), 2 * NG)
    for b in range(rows):
        j = ((r ^ b) * wide + iota((1, wide), 1)).astype(jnp.float32)
        later[2, b : b + 1, :] = 1.0 / (1.0 - BEAM_SLOPE * (j + 0.5) / FS)


def turns(scale, chunks, width, wide, offs, order, roff, after):
    rows = roff.shape[0]
    height = -(-rows // TILE) * TILE
    *waves, turned, later = pl.pallas_call(
        functools.partial(turn_kernel, scale, chunks),
        in_specs=[HBM] * 4,
        out_specs=[VMEM] * (chunks + 2),
        out_shape=[jax.ShapeDtypeStruct((width // chunks, wide), jnp.bfloat16)] * chunks
        + [
            jax.ShapeDtypeStruct((2 * rows, height, width), jnp.float32),
            jax.ShapeDtypeStruct((3, height, wide), jnp.float32),
        ],
        scratch_shapes=[pltpu.SMEM(x.shape, x.dtype) for x in (offs, order, roff)] + [pltpu.SemaphoreType.DMA((3,))],
        compiler_params=pltpu.CompilerParams(vmem_limit_bytes=16 * MIB),
        cost_estimate=pl.CostEstimate(flops=10**9, bytes_accessed=4 * width * wide, transcendentals=0),
        name="turns",
    )(after, *in_hbm(offs, order, roff))
    return waves, turned, later


def pair_kernel(parts, mine, *refs):
    taken, total, sent = refs[:parts], refs[parts], refs[parts + 1 :]
    high, width = total.shape
    piece = width // parts
    for n in range(parts):
        to = slice(n * piece, (n + 1) * piece)
        total[:, to] = mine[:high, to] + taken[n][:high].astype(jnp.float32)
        for k, out in enumerate(sent):
            at = slice((k + 1) * high, (k + 2) * high)
            out[:, to] = (mine[at, to] + taken[n][at].astype(jnp.float32)).astype(out.dtype)


def pair_sum(slots, mine, taken):
    rows, width = mine.shape
    high = rows // slots
    return pl.pallas_call(
        functools.partial(pair_kernel, len(taken)),
        in_specs=[VMEM] * (1 + len(taken)),
        out_specs=[VMEM] * slots,
        out_shape=[jax.ShapeDtypeStruct((high, width), jnp.float32)]
        + [jax.ShapeDtypeStruct((high, width), jnp.bfloat16)] * (slots - 1),
        compiler_params=pltpu.CompilerParams(vmem_limit_bytes=8 * MIB),
        name="pair",
    )(mine, *taken)


def sum_kernel(arrived, total, *refs):
    taken, outs = refs[:arrived], refs[arrived:]
    double, _ = outs[0].shape
    high = double // 2
    rows = len(outs)
    span = high * rows
    r = lax.axis_index("row")

    def rows_at(at):
        value = total[at, :]
        for other in taken:
            value = value + other[at, :].astype(jnp.float32)
        return value

    for p in range(rows):
        for z in range(2):
            if high % TILE == 0:
                at = pl.ds(pl.multiple_of(z * span + (r ^ p) * high, high), high)
                outs[p][z * high : (z + 1) * high, :] = rows_at(at).astype(outs[p].dtype)
    if high % TILE != 0:
        value = rows_at(slice(0, 2 * span))
        for p in range(rows):
            parts = []
            for z in range(2):
                part = value[z * span : z * span + high]
                for q in range(1, rows):
                    at = z * span + q * high
                    part = jnp.where((r ^ p) == q, value[at : at + high], part)
                parts.append(part)
            outs[p][...] = jnp.concatenate(parts, axis=0).astype(outs[p].dtype)


def sum_of(rows, total, taken):
    depth = total.shape[1]
    return pl.pallas_call(
        functools.partial(sum_kernel, len(taken)),
        in_specs=[VMEM] * (len(taken) + 1),
        out_specs=[VMEM] * rows,
        out_shape=[jax.ShapeDtypeStruct((total.shape[0] // rows, depth), jnp.bfloat16)] * rows,
        compiler_params=pltpu.CompilerParams(vmem_limit_bytes=16 * MIB),
        name="sum",
    )(total, *taken)


def row_kernel(rows, first, earlier, last, wave, turned, later, *refs):
    pieces, refs = refs[:rows], refs[rows:]
    before, refs = refs[:earlier], refs[earlier:]
    outs, left = refs[:-1], refs[-1]
    double, span = pieces[0].shape
    high = double // 2
    width = wave.shape[1]
    half = span // 2
    mirror = jnp.where(iota((half, half), 0) + iota((half, half), 1) == half - 1, 1.0, 0.0).astype(jnp.bfloat16)
    firsts = jnp.concatenate([pieces[p][:, :half] for p in range(rows)], axis=0)
    firsts = jnp.dot(firsts, mirror, preferred_element_type=jnp.float32)
    for p in range(rows):
        near = firsts[p * double : (p + 1) * double]
        far = pieces[p][:, half:].astype(jnp.float32)
        for b in range(rows):

            def turn(value, at):
                factor = (turned[2 * p + z, b : b + 1, first + at : first + at + half] for z in range(2))
                factor = tuple(jnp.broadcast_to(v, (high, half)) for v in factor)
                return times((value[:high], value[high:]), factor)

            x, y = turn(near, 0), turn(far, half)
            even = (y[0] + x[0], y[1] + x[1])
            odd = (y[0] - x[0], y[1] - x[1])
            at = (p * rows + b) * double
            left[at : at + high, :half] = even[0].astype(left.dtype)
            left[at : at + high, half:] = (-odd[1]).astype(left.dtype)
            left[at + high : at + double, :half] = even[1].astype(left.dtype)
            left[at + high : at + double, half:] = odd[0].astype(left.dtype)
    piece = min(2 * LANES, width)
    largest = jnp.zeros((high, LANES), jnp.float32)
    for n in range(0, width, piece):
        product = jnp.dot(left[...], wave[:, n : n + piece], preferred_element_type=jnp.float32)
        if earlier:
            product = product + before[0][:, n : n + piece]
        if not last:
            outs[0][:, n : n + piece] = product
            continue
        for b in range(rows):
            real = imag = None
            for p in range(rows):
                at = (p * rows + b) * double
                value = (product[at : at + high], product[at + high : at + double])
                turn = tuple(later[z, p : p + 1, n : n + piece] for z in range(2))
                x, y = times(value, turn)
                real = x if real is None else real + x
                imag = y if imag is None else imag + y
            beam = later[2, b : b + 1, n : n + piece]
            real = real * beam
            imag = imag * beam
            power = real * real + imag * imag
            both = jnp.concatenate([real, imag], axis=0).astype(jnp.bfloat16)
            for m in range(0, piece, LANES):
                at = (n + m) // LANES * double
                outs[b][at : at + double] = both[:, m : m + LANES]
                largest = jnp.maximum(largest, power[:, m : m + LANES])
    if not last:
        return
    peak = jnp.broadcast_to(jnp.sqrt(jnp.max(largest, keepdims=True)), (2 * TILE, LANES))
    one = peak.astype(jnp.bfloat16).astype(jnp.float32)
    two = (peak - one).astype(jnp.bfloat16).astype(jnp.float32)
    three = peak - one - two
    sub = iota((2 * TILE, LANES), 0)
    peak = jnp.where(sub == 0, one, jnp.where(sub == 1, two, jnp.where(sub == 2, three, 0.0)))
    for b in range(rows):
        outs[b][width // LANES * double :] = peak.astype(jnp.bfloat16)


def rows_of(first, last, pieces, wave, turned, later, before):
    rows = len(pieces)
    double, span = pieces[0].shape
    width = wave.shape[1]
    if last:
        shape = [jax.ShapeDtypeStruct((width // LANES * double + 2 * TILE, LANES), jnp.bfloat16)] * rows
    else:
        shape = [jax.ShapeDtypeStruct((rows * rows * double, width), jnp.float32)]
    return pl.pallas_call(
        functools.partial(row_kernel, rows, first, len(before), last),
        in_specs=[VMEM] * (rows + 3 + len(before)),
        out_specs=[VMEM] * len(shape),
        out_shape=shape,
        scratch_shapes=[pltpu.VMEM((rows * rows * double, span), jnp.bfloat16)],
        compiler_params=pltpu.CompilerParams(vmem_limit_bytes=24 * MIB),
        cost_estimate=pl.CostEstimate(
            flops=rows * rows * double * 2 * span * width, bytes_accessed=2 * span * width, transcendentals=0
        ),
    )(wave, turned, later, *pieces, *before)


def finish_kernel(rows, chunks, *refs):
    pieces, (image, peak) = refs[:rows], refs[rows:]
    width = image.shape[3]
    high = image.shape[2] // (rows * chunks)
    tall = width // LANES * 2 * high
    r = lax.axis_index("row")
    largest = None
    for p in range(rows):
        for h in range(chunks):
            for n in range(0, width, LANES):
                row = h * tall + n // LANES * 2 * high
                if high % TILE == 0:
                    at = pl.ds(pl.multiple_of((h * rows + (r ^ p)) * high, high), high)
                    value = pieces[p][row : row + 2 * high, :].astype(jnp.float32)
                else:
                    at = pl.ds((h * rows + p) * high, high)
                    value = pieces[0][row : row + 2 * high, :].astype(jnp.float32)
                    for q in range(1, rows):
                        other = pieces[q][row : row + 2 * high, :].astype(jnp.float32)
                        value = jnp.where((r ^ p) == q, other, value)
                image[0, 0, at, n : n + LANES] = value[:high]
                image[0, 1, at, n : n + LANES] = value[high:]
        parts = pieces[p][chunks * tall :, :].astype(jnp.float32)
        value = (parts[0:1] + parts[1:2]) + parts[2:3]
        largest = value if largest is None else jnp.maximum(largest, value)
    peak[0] = jnp.max(largest)


def finish(pieces, chunks, width):
    rows = len(pieces)
    return pl.pallas_call(
        functools.partial(finish_kernel, rows, chunks),
        in_specs=[VMEM] * rows,
        out_specs=[VMEM, SMEM],
        out_shape=[
            jax.ShapeDtypeStruct((1, 2, FR, width), jnp.float32),
            jax.ShapeDtypeStruct((1,), jnp.float32),
        ],
        compiler_params=pltpu.CompilerParams(vmem_limit_bytes=16 * MIB),
        name="finish",
    )(*pieces)


def step(visibilities, col_offsets, row_offsets, facet_offsets, facet_order, vis_counts):
    cols = lax.axis_size("col")
    rows = lax.axis_size("row")
    _, depth, width = visibilities.shape
    slots = cols // 2
    wide = FS // rows
    chunks = 2
    span = width // chunks
    half = span // 2

    def swap(value, axis, count, bit):
        return lax.ppermute(value, axis, [(i, i ^ bit) for i in range(count)])

    given, kept, other, small = first_columns(
        slots, span, 1.0 / math.sqrt(depth * cols), facet_offsets.T, facet_order, col_offsets, vis_counts, visibilities
    )
    totals, sents = [], []
    for h in range(chunks):
        blocks = blocks_of(h, half, width)
        if h == 0:
            taken = [swap(given, "col", cols, 1)]
            mine, own = own_columns(slots, blocks, half, small, kept, given)
        else:
            taken = []
            for n, block in enumerate(blocks):
                given = more_columns((block,), half, jnp.bfloat16, other, kept, given if n else totals[h - 1])
                taken.append(swap(given, "col", cols, 1))
            mine = more_columns(blocks, half, jnp.float32, own, kept, given)
        total, *sent = pair_sum(slots, mine, taken)
        totals.append(total)
        sents.append([swap(value, "col", cols, 2 * k + 2) for k, value in enumerate(sent)])
    pieces = []
    for h in range(chunks):
        mine, *others = sum_of(rows, totals[h], sents[h])
        pieces.append([mine] + [swap(value, "row", rows, p + 1) for p, value in enumerate(others)])
    waves, turned, later = turns(
        0.5 / math.sqrt(width * rows), chunks, width, wide, facet_offsets.T, facet_order, row_offsets, pieces[0][0]
    )
    parts = []
    for h in range(chunks):
        parts = rows_of(h * span, h == chunks - 1, pieces[h], waves[h], turned, later, parts)
    far = [swap(part, "row", rows, p) for p, part in reversed(list(enumerate(parts))) if p > 0]
    parts = [parts[0]] + far[::-1]
    return tuple(finish(parts, 1, wide))


def solution(mesh):
    in_specs = (P(None, "col", "row"), P("col"), P(), P(), P(), P("col", "row"))
    out_specs = (P("col", None, None, "row"), P("col"))
    return jax.shard_map(step, mesh=mesh, in_specs=in_specs, out_specs=out_specs, check_vma=False)
```
